512 devices in a mesh: shear: 64 (over z_hi, y, x), cross: 8 (over z_lo, core).
Axes of the slice: x: 4, y: 8, z: 8 (z_hi: 2, z_lo: 4; z = z_hi * 4 + z_lo), core: 2. Of those that a mesh axis runs over, the one named last changes fastest.
Arguments:
- positions: float32 [3, 64, 16, 8, 256], P(None, 'shear', None, 'cross'), may hold values from 0 to 1
- masses: float32 [64, 16, 8, 256], P('shear', None, 'cross'), may hold values from 0.002 to 0.008
- counts: int32 [64, 16, 8], P('shear', None, 'cross'), may hold values from 32 to 256
- shear_offset: int32 [1], replicated, may hold values from 0 to 15
Outputs:
- density: float32 [64, 16, 8, 256], P('shear', None, 'cross')
The draws below stay inside these ranges and needn't reach their ends.
Inputs may be any that keep to these rules, and one draw needn't show every extreme that they name: `shear_offset`: a whole number of cells.
All inputs are finite; a program needn't handle non-finite values.
Results may differ from the reference program's by a relative error of at most 0.0003.
Values sent between devices are 32-bit elements; how exact they have to be, the bound alone decides.
No kernel may reach another device: no remote copies, remote signals or barrier semaphores. Data moves between devices by JAX's collectives and lax.ppermute only.
A program may use at most 64 MiB of HBM per device.

```python
import math
import jax
import jax.numpy as jnp
from jax import lax

P_SIZE = 256
NX = 16
NY = 64
NZ = 8


def place_ends(entries, stream_key, least, largest):
    index_at = [jax.random.randint(jax.random.fold_in(stream_key, axis), (), 0, length) for axis, length in enumerate(entries.shape)]
    main_axis = entries.shape.index(max(entries.shape))
    next_to = index_at[:main_axis] + [(index_at[main_axis] + 1) % entries.shape[main_axis]] + index_at[main_axis + 1:]
    return entries.at[tuple(index_at)].set(least).at[tuple(next_to)].set(largest)


def level_of(own_key, dims, pieces, least, largest):
    level = 1.0
    for position, blocks in pieces:
        heights = jax.random.uniform(jax.random.fold_in(jax.random.fold_in(own_key, 6), position), (blocks,), jnp.float32, least / len(pieces), largest / len(pieces))
        level = level * jnp.repeat(jnp.exp(heights), dims[position] // blocks).reshape((-1,) + (1,) * (len(dims) - 1 - position))
    return level


def setup_inputs(seed: int = 0) -> dict:
    splits = jax.random.split(jax.random.key(seed), 5)
    positions = jnp.clip(1.0 * jax.random.uniform(splits[0], (3, NY, NX, NZ, P_SIZE), jnp.float32) ** level_of(splits[0], (3, NY, NX, NZ, P_SIZE), ((1, 64), (3, 8)), -0.2, 0.2), 0.0, 1.0)
    masses = jnp.clip(jnp.exp(math.log(0.008) - 1.3862944 * jax.random.uniform(splits[1], (NY, NX, NZ, P_SIZE), jnp.float32) ** level_of(splits[1], (NY, NX, NZ, P_SIZE), ((0, 64), (2, 8)), -0.2, 0.2)), 0.002, 0.008)
    counts = place_ends(jax.random.randint(splits[2], (NY, NX, NZ), P_SIZE // 8, P_SIZE + 1), jax.random.fold_in(splits[2], 1), P_SIZE // 8, P_SIZE).astype(jnp.int32)
    shear_offset = jax.random.randint(splits[3], (1,), 0, NX).astype(jnp.int32)
    return dict(positions=positions, masses=masses, counts=counts, shear_offset=shear_offset)


def spline(squared):
    radius = jnp.sqrt(squared) * 4.0
    inner_part = 1.0 - 1.5 * radius * radius + 0.75 * radius * radius * radius
    outer_part = 0.25 * jnp.maximum(2.0 - radius, 0.0) ** 3
    return jnp.where(radius < 1.0, inner_part, outer_part) * (64.0 / 3.141592653589793)

def distance_sq(target, source_pos, offset_vec):
    squared = None
    for component in range(3):
        moved = source_pos[component] + offset_vec[component]
        gap = target[component][..., :, None] - moved[..., None, :]
        squared = gap * gap if squared is None else squared + gap * gap
    return squared

def reference(positions, masses, counts, shear_offset):
    slot_index = lax.broadcasted_iota(jnp.int32, masses.shape, 3)
    is_valid = slot_index < counts[..., None]
    weight = jnp.where(is_valid, masses, jnp.float32(0.0))
    particle_data = jnp.concatenate([positions, weight[None]], 0)
    offset = shear_offset[0]
    top_row = jnp.roll(particle_data[:, 0:1], -offset, axis=2)
    bottom_row = jnp.roll(particle_data[:, -1:], offset, axis=2)
    extended = jnp.concatenate([bottom_row, particle_data, top_row], 1)
    extended = jnp.concatenate([extended[:, :, :, -1:], extended, extended[:, :, :, :1]], 3)
    width_z = masses.shape[2]

    def row_density(row_at):
        band = lax.dynamic_slice_in_dim(extended, row_at, 3, 1)
        target = band[:3, 1, :, 1:1 + width_z]
        density = jnp.zeros(target.shape[1:], jnp.float32)
        for step_y in (-1, 0, 1):
            for step_z in (-1, 0, 1):
                for step_x in (-1, 0, 1):
                    source_cells = jnp.roll(band[:, 1 + step_y, :, 1 + step_z:1 + step_z + width_z], -step_x, axis=1)
                    offset_vec = (float(step_y), float(step_x), float(step_z))
                    kernel = spline(distance_sq(target, source_cells[:3], offset_vec))
                    density = density + lax.optimization_barrier(jnp.sum(kernel * source_cells[3][..., None, :], axis=-1))
        valid_row = lax.dynamic_index_in_dim(is_valid, row_at, 0, keepdims=False)
        return jnp.where(valid_row, density, jnp.float32(0.0))
    return lax.map(row_density, jnp.arange(masses.shape[0], dtype=jnp.int32))
```

```python
import functools

import jax
import jax.numpy as jnp
import numpy as np
from jax import lax
from jax.experimental import pallas as pl
from jax.experimental.pallas import tpu as pltpu
from jax.sharding import PartitionSpec as P

NX = 16
PS = 256
ROWS = 4480
NULL_ROW = 4416
BLOCK = 32
GROUP = 8
GAP = 48
RC = 24
STRIDE = 33
KD = 32
F32 = jnp.float32
BF16 = jnp.bfloat16

FULL = [(0, 0), (0, 1), (0, 2), (1, 0), (1, 1), (1, 2), (2, 0), (2, 1)]
SHORT = [(0, 0), (0, 1), (0, 2), (1, 0), (1, 1), (2, 0)]


def constants():
    j = np.arange(128)
    bins, cell = j // 16, j % 16
    quad, half = bins // 2, bins % 2
    place = 2 * cell + half
    rows = np.zeros((200, 128), np.float32)
    for q in range(4):
        for r in range(18):
            low, high = max(2 * (r - 1) - 1, 0), min(2 * (r - 1) + 3, 32)
            rows[q * RC + r] = (quad == q) & (place < low)
            rows[96 + q * RC + r] = (quad == q) & (place < high)
        rows[192 + q] = quad == q
    lanes = np.zeros((128, 256), np.float32)
    for q in range(4):
        for x in range(16):
            lanes[:, q * 16 + x] = (cell == x) & (quad < q)
            lanes[:, 64 + q * 16 + x] = (cell == x) & (quad == q)
            lanes[:, 128 + q * 16 + x] = (quad == q) & (cell < x)
    return jnp.asarray(rows, BF16), jnp.asarray(lanes, BF16)


def pieces(value):
    first = value.astype(BF16).astype(F32)
    rest = value - first
    second = rest.astype(BF16).astype(F32)
    return first, second, rest - second


def dot(a, b, dims=((1,), (0,))):
    return lax.dot_general(a, b, (dims, ((), ())), preferred_element_type=F32)


def prep_kernel(data, mrows, mlanes, t_out, rank_out, list_out, feat0, feat1, sorted_s, t_s, meta_v, meta_s, sem):
    y, x, z, m = data[0], data[1], data[2], data[3]
    valid = m > 0.0
    one = jnp.float32(1.0)
    nil = jnp.float32(0.0)
    code = jnp.where(y >= 0.5, 4.0, 0.0) + jnp.where(z >= 0.5, 2.0, 0.0) + jnp.where(x >= 0.5, 1.0, 0.0)
    code = jnp.where(valid, code, 9.0)
    masks = [jnp.where(code == float(b), one, nil) for b in range(8)]
    stacked = jnp.concatenate(masks, 0).astype(BF16)
    row_i = lax.broadcasted_iota(jnp.int32, (PS, PS), 0)
    lane_i = lax.broadcasted_iota(jnp.int32, (PS, PS), 1)
    upper = jnp.where(row_i <= lane_i, one, nil).astype(BF16)
    running = dot(stacked, upper)
    total = dot(stacked, jnp.ones((PS, 128), BF16))
    begin = jnp.zeros((16, 128), F32)
    rank = jnp.zeros((16, PS), F32)
    for b in range(8):
        wide = jnp.concatenate([begin, begin], 1)
        rank = rank + masks[b] * (wide + running[b * 16 : b * 16 + 16] - 1.0)
        begin = begin + total[b * 16 : b * 16 + 16]
    rank = jnp.where(valid, rank, -1.0)
    rank_out[...] = rank

    columns = dot(mrows[...], total.astype(BF16))
    base = [jnp.zeros((1, 128), F32)]
    for q in range(3):
        end = base[q] + columns[192 + q : 193 + q] + float(GAP + 15)
        base.append(jnp.floor(end * 0.0625) * 16.0)
    base_col = jnp.concatenate([jnp.broadcast_to(b, (RC, 128)) for b in base], 0)
    low, high = columns[0:96], columns[96:192]
    first = jnp.floor((low + base_col) * 0.0625) * 16.0
    n_blocks = jnp.floor((high + base_col - first + float(BLOCK - 1)) * (1.0 / BLOCK))
    n_blocks = jnp.where(high > low, n_blocks, 0.0)
    gi = lax.broadcasted_iota(jnp.int32, (96, 96), 0)
    gj = lax.broadcasted_iota(jnp.int32, (96, 96), 1)
    before = dot(jnp.where(gj < gi, one, nil).astype(BF16), n_blocks.astype(BF16))
    g128 = lax.broadcasted_iota(jnp.int32, (RC, 128), 0)
    tag = jnp.concatenate([(g128 + 32 * q).astype(F32) for q in range(4)], 0)
    null = float(NULL_ROW * 128 + 23)
    lane96 = lax.broadcasted_iota(jnp.int32, (96, 128), 1).astype(F32)
    out_rows = []
    for t in range(4):
        away = lane96 + float(128 * t) - before
        inside = (away >= 0.0) & (away < n_blocks)
        entry = (first + away * float(BLOCK)) * 128.0 + tag - null
        out_rows.append(jnp.sum(jnp.where(inside, entry, 0.0), 0, keepdims=True) + null)
    out_rows.append(before[95:96] + n_blocks[95:96])
    total_row = dot(jnp.ones((8, PS), BF16), stacked, ((1,), (1,)))
    meta = dot(total_row.astype(BF16), mlanes[...])
    lane1 = lax.broadcasted_iota(jnp.int32, (1, 128), 1)
    base_lane = jnp.where(lane1 < 16, base[0], jnp.where(lane1 < 32, base[1], jnp.where(lane1 < 48, base[2], base[3])))
    out_rows.append(meta[0:1, 0:128])
    out_rows.append(meta[0:1, 128:256] + base_lane)
    out_rows.append(jnp.zeros((1, 128), F32))
    table = jnp.concatenate(out_rows, 0).astype(jnp.int32)
    list_out[...] = table
    meta_v[...] = table
    copy = pltpu.make_async_copy(meta_v, meta_s, sem)
    copy.start()

    cell_i = lax.broadcasted_iota(jnp.int32, (16, PS), 0).astype(F32)
    xg = x + (cell_i - 8.0)
    norm = y * y + xg * xg + z * z
    py, pz, px, pn = pieces(y), pieces(z), pieces(xg), pieces(norm)
    features = [py[a] for a, _ in SHORT] + [pz[a] for a, _ in SHORT] + [px[a] for a, _ in FULL] + [pn[a] for a, _ in FULL]
    ones = jnp.ones((16, PS), F32)
    features = features + [ones, ones, ones, jnp.zeros((16, PS), F32)]
    for k in range(KD):
        feat0[pl.ds(k, 16, stride=STRIDE), :] = features[k][:, 0:128]
        feat1[pl.ds(k, 16, stride=STRIDE), :] = features[k][:, 128:256]
    t_s[...] = jnp.zeros(t_s.shape, F32)
    row_f = row_i.astype(F32)
    for c in range(16):
        place = jnp.where(row_f == rank[c : c + 1], one, nil).astype(BF16)
        both = jnp.concatenate([feat0[c * STRIDE : c * STRIDE + KD, :], feat1[c * STRIDE : c * STRIDE + KD, :]], 1)
        sorted_s[c, 0:PS, :] = dot(place, both.astype(BF16), ((1,), (1,)))
        sorted_s[c, PS : PS + 64, :] = jnp.zeros((64, KD), F32)
    copy.wait()
    for q in range(4):

        def append(c, carry, q=q):
            source = meta_s[5, q * 16 + c]
            count = meta_s[5, 64 + q * 16 + c]
            target = meta_s[6, q * 16 + c]

            def chunk(i, carry):
                t_s[pl.ds(target + 64 * i, 64), :] = sorted_s[c, pl.ds(source + 64 * i, 64), :]
                return carry

            return lax.fori_loop(0, (count + 63) // 64, chunk, carry)

        lax.fori_loop(0, 16, append, 0)
    t_out[...] = t_s[...].astype(BF16)


def pair_kernel(pencils, first_of, second_of, n_in, *refs):
    n = len(pencils)
    table, shift = refs[0], refs[1]
    inputs = refs[2 : 2 + n_in]
    targets, rank_ref, partial = refs[2 + n_in : 5 + n_in]
    out, roll_s, stage0, stage1, weights, c_lo, c_hi, acc1, acc2, d_a, d_b, back = refs[5 + n_in :]
    row_i = lax.broadcasted_iota(jnp.int32, (RC, PS), 0).astype(F32)
    acc1[...] = jnp.zeros(acc1.shape, F32)
    acc2[...] = jnp.zeros(acc2.shape, F32)
    for p, (which, index, dy, dz) in enumerate(pencils):
        start = 15 if dy == 0 else lax.rem(shift[0 if dy < 0 else 1] + 15, 16)
        rolled = []
        for f in range(4):
            value = inputs[which][index, f]
            for half in range(2):
                part = value[:, half * 128 : half * 128 + 128]
                for copy in range(3):
                    roll_s[p, 2 * f + half, copy * 16 : copy * 16 + 16, :] = part
            rolled.append(
                jnp.concatenate([roll_s[p, 2 * f, pl.ds(start, RC), :], roll_s[p, 2 * f + 1, pl.ds(start, RC), :]], 1)
            )
        y, x, z, m = rolled
        y = y + float(dy)
        z = z + float(dz)
        x = x + (row_i - 9.0)
        live = (m > 0.0) & (row_i < 18.0)
        cube = jnp.where(live, m, 1.0) * (16.0 / 3.141592653589793)
        c = jnp.where(live, jnp.exp2(jnp.log2(cube) * (1.0 / 3.0)), 0.0)
        w = c * c * 16.0
        norm = w * (y * y + x * x + z * z)
        w2 = w * -2.0
        py, pz, px, pw, pn = pieces(y * w2), pieces(z * w2), pieces(x * w2), pieces(w), pieces(norm)
        features = [py[b] for _, b in SHORT] + [pz[b] for _, b in SHORT] + [px[b] for _, b in FULL] + [pw[b] for _, b in FULL]
        features = features + list(pn) + [jnp.zeros((RC, PS), F32)]
        for k in range(KD):
            stage0[p, pl.ds(k, RC, stride=STRIDE), :] = features[k][:, 0:128]
            stage1[p, pl.ds(k, RC, stride=STRIDE), :] = features[k][:, 128:256]
        c_lo[pl.ds(p * RC, RC), :] = c[:, 0:128]
        c_hi[pl.ds(p * RC, RC), :] = c[:, 128:256]
        for r in range(RC):
            if r < 18 or r == 23:
                weights[p * RC + r, :, 0:128] = stage0[p, r * STRIDE : r * STRIDE + KD, :].astype(BF16)
                weights[p * RC + r, :, 128:256] = stage1[p, r * STRIDE : r * STRIDE + KD, :].astype(BF16)

    def decode(i):
        entry = table[lax.shift_right_logical(i, 7), lax.bitwise_and(i, 127)]
        at = pl.multiple_of(lax.shift_left(lax.shift_right_logical(entry, 11), 4), 16)
        q = lax.bitwise_and(lax.shift_right_logical(entry, 5), 3)
        r = lax.bitwise_and(entry, 31)
        return at, first_of(q) * RC + r, second_of(q) * RC + r

    def multiply(i, slot):
        at, w_a, w_b = decode(i)
        lhs = targets[pl.ds(at, BLOCK), :]
        slot[:, 0:256] = dot(lhs, weights[w_a])
        slot[:, 256:512] = dot(lhs, weights[w_b])

    def consume(i, slot):
        at, w_a, w_b = decode(i)
        cs = []
        for ref, w in ((c_lo, w_a), (c_hi, w_a), (c_lo, w_b), (c_hi, w_b)):
            cs.append(ref[pl.ds(w, 8, stride=0), :])
        for g in range(BLOCK // 8):
            sum1 = acc1[pl.ds(at + 8 * g, 8), :]
            sum2 = acc2[pl.ds(at + 8 * g, 8), :]
            for t in range(4):
                square = jnp.maximum(slot[8 * g : 8 * g + 8, 128 * t : 128 * t + 128], 1e-30)
                root = square * lax.rsqrt(square)
                inner = cs[t] - root
                outer = jnp.maximum(inner + cs[t], 0.0)
                inner = jnp.maximum(inner, 0.0)
                sum1 = sum1 + outer * outer * outer
                sum2 = sum2 + inner * inner * inner
            acc1[pl.ds(at + 8 * g, 8), :] = sum1
            acc2[pl.ds(at + 8 * g, 8), :] = sum2

    count = table[4, 0]
    for k in range(GROUP // 2):
        multiply(k, d_a.at[k])

    def step(it, carry):
        i = it * GROUP
        half = GROUP // 2
        for k in range(half):
            multiply(i + half + k, d_b.at[k])
        for k in range(half):
            consume(i + k, d_a.at[k])
        for k in range(half):
            multiply(i + GROUP + k, d_a.at[k])
        for k in range(half):
            consume(i + half + k, d_b.at[k])
        return carry

    lax.fori_loop(0, (count + GROUP - 1) // GROUP, step, 0)

    for q in range(4):

        def fetch(c, carry, q=q):
            target = table[5, q * 16 + c]
            length = table[5, 64 + q * 16 + c]
            source = table[6, q * 16 + c]

            def chunk(i, carry):
                value = acc1[pl.ds(source + 64 * i, 64), :] - 4.0 * acc2[pl.ds(source + 64 * i, 64), :]
                back[c, pl.ds(target + 64 * i, 64), :] = value
                return carry

            return lax.fori_loop(0, (length + 63) // 64, chunk, carry)

        if q == 0:
            back[...] = jnp.zeros(back.shape, F32)
        lax.fori_loop(0, 16, fetch, 0)
    row_f = lax.broadcasted_iota(jnp.int32, (PS, PS), 0).astype(F32)
    row8 = lax.broadcasted_iota(jnp.int32, (8, PS), 0)
    ones = jnp.ones((8, 128), BF16)
    for c in range(16):
        value = back[c, 0:PS, :]
        high = value.astype(BF16)
        low = (value - high.astype(F32)).astype(BF16)
        sums = dot(ones, high, ((1,), (1,))) + dot(ones, low, ((1,), (1,)))
        s1, s2, s3 = pieces(sums)
        lhs = jnp.where(row8 == 0, s1, jnp.where(row8 == 1, s2, jnp.where(row8 == 2, s3, 0.0))).astype(BF16)
        place = jnp.where(row_f == rank_ref[c : c + 1, :], 1.0, 0.0).astype(BF16)
        spread = jnp.sum(dot(lhs, place), 0, keepdims=True)
        out[c : c + 1, :] = spread + partial[c : c + 1, :]


VMEM_SPEC = pl.BlockSpec(memory_space=pltpu.VMEM)
SMEM_SPEC = pl.BlockSpec(memory_space=pltpu.SMEM)


def prepare(data, interpret=False):
    mrows, mlanes = constants()
    return pl.pallas_call(
        prep_kernel,
        out_shape=(
            jax.ShapeDtypeStruct((ROWS, KD), BF16),
            jax.ShapeDtypeStruct((NX, PS), F32),
            jax.ShapeDtypeStruct((8, 128), jnp.int32),
        ),
        in_specs=[VMEM_SPEC] * 3,
        out_specs=[VMEM_SPEC] * 3,
        scratch_shapes=[
            pltpu.VMEM((16 * STRIDE, 128), F32),
            pltpu.VMEM((16 * STRIDE, 128), F32),
            pltpu.VMEM((16, PS + 64, KD), F32),
            pltpu.VMEM((ROWS, KD), F32),
            pltpu.VMEM((8, 128), jnp.int32),
            pltpu.SMEM((8, 128), jnp.int32),
            pltpu.SemaphoreType.DMA,
        ],
        compiler_params=pltpu.CompilerParams(vmem_limit_bytes=40 << 20),
        interpret=interpret,
        name="prepare",
    )(data, mrows, mlanes)


def pair_sums(pencils, first_of, second_of, table, shift, inputs, targets, rank, partial, name, interpret=False):
    n = len(pencils)
    return pl.pallas_call(
        functools.partial(pair_kernel, pencils, first_of, second_of, len(inputs)),
        out_shape=jax.ShapeDtypeStruct((NX, PS), F32),
        in_specs=[SMEM_SPEC] * 2 + [VMEM_SPEC] * (len(inputs) + 3),
        out_specs=VMEM_SPEC,
        scratch_shapes=[
            pltpu.VMEM((n, 8, 48, 128), F32),
            pltpu.VMEM((n, RC * STRIDE, 128), F32),
            pltpu.VMEM((n, RC * STRIDE, 128), F32),
            pltpu.VMEM((n * RC, KD, PS), BF16),
            pltpu.VMEM((n * RC, 128), F32),
            pltpu.VMEM((n * RC, 128), F32),
            pltpu.VMEM((ROWS, 128), F32),
            pltpu.VMEM((ROWS, 128), F32),
            pltpu.VMEM((GROUP // 2, BLOCK, 512), F32),
            pltpu.VMEM((GROUP // 2, BLOCK, 512), F32),
            pltpu.VMEM((NX, PS + 64, 128), F32),
        ],
        compiler_params=pltpu.CompilerParams(vmem_limit_bytes=40 << 20),
        interpret=interpret,
        name=name,
    )(table, shift, *inputs, targets, rank, partial)


PENCILS_A = ((0, 0, 0, 0), (0, 1, -1, 0), (0, 2, 1, 0))
PENCILS_B = ((0, 0, 0, -1), (1, 0, 0, 1), (0, 1, -1, -1), (1, 1, -1, 1), (0, 2, 1, -1), (1, 2, 1, 1))


def near_sums(table, shift, rows, targets, rank, interpret=False):
    zero = jnp.zeros((NX, PS), F32)
    return pair_sums(
        PENCILS_A, lambda q: 0, lambda q: 1 + lax.shift_right_logical(q, 1), table, shift, [rows], targets, rank, zero, "near", interpret
    )


def far_sums(table, shift, low, high, targets, rank, partial, interpret=False):
    return pair_sums(
        PENCILS_B, lambda q: lax.bitwise_and(q, 1), lambda q: 2 + q, table, shift, [low, high], targets, rank, partial, "far", interpret
    )


def ring(axis, distance):
    count = lax.axis_size(axis)
    return [(i, (i + distance) % count) for i in range(count)]


def shards(positions, masses, counts, shear_offset):
    slot_index = lax.broadcasted_iota(jnp.int32, masses.shape, 3)
    weight = jnp.where(slot_index < counts[..., None], masses, jnp.float32(0.0))
    data = jnp.concatenate([positions, weight[None]], 0).reshape(4, NX, PS)
    index = lax.axis_index("shear")
    offset = shear_offset[0]
    shift = jnp.stack([
        jnp.where(index == 0, NX - offset, 0),
        jnp.where(index == lax.axis_size("shear") - 1, offset, 0),
    ]).astype(jnp.int32)
    below = lax.ppermute(data, "shear", ring("shear", 1))
    above = lax.ppermute(data, "shear", ring("shear", -1))
    targets, rank, table = prepare(data)
    rows = jnp.stack([data, below, above])
    low = lax.ppermute(rows, "cross", ring("cross", 1))
    high = lax.ppermute(rows, "cross", ring("cross", -1))
    partial = near_sums(table, shift, rows, targets, rank)
    density = far_sums(table, shift, low, high, targets, rank, partial)
    return density.reshape(masses.shape)


def solution(mesh):
    in_specs = (
        P(None, "shear", None, "cross", None),
        P("shear", None, "cross", None),
        P("shear", None, "cross"),
        P(),
    )
    out_specs = P("shear", None, "cross", None)
    return jax.shard_map(shards, mesh=mesh, in_specs=in_specs, out_specs=out_specs, check_vma=False)
```

```python
import functools

import jax
import jax.numpy as jnp
import numpy as np
from jax import lax
from jax.experimental import pallas as pl
from jax.experimental.pallas import tpu as pltpu
from jax.sharding import PartitionSpec as P

NX = 16
PS = 256
ROWS = 4480
NULL_ROW = 4416
BLOCK = 32
GROUP = 16
GAP = 48
MOVE = 96
RC = 24
STRIDE = 33
KD = 32
F32 = jnp.float32
BF16 = jnp.bfloat16

FULL = [(0, 0), (0, 1), (0, 2), (1, 0), (1, 1), (1, 2), (2, 0), (2, 1)]
SHORT = [(0, 0), (0, 1), (0, 2), (1, 0), (1, 1), (2, 0)]


def constants():
    j = np.arange(128)
    bins, cell = j // 16, j % 16
    quad, half = bins // 2, bins % 2
    place = 2 * cell + half
    rows = np.zeros((200, 128), np.float32)
    for q in range(4):
        for r in range(18):
            low, high = max(2 * (r - 1) - 1, 0), min(2 * (r - 1) + 3, 32)
            rows[q * RC + r] = (quad == q) & (place < low)
            rows[96 + q * RC + r] = (quad == q) & (place < high)
        rows[192 + q] = quad == q
    lanes = np.zeros((128, 256), np.float32)
    for q in range(4):
        for x in range(16):
            lanes[:, q * 16 + x] = (cell == x) & (quad < q)
            lanes[:, 64 + q * 16 + x] = (cell == x) & (quad == q)
            lanes[:, 128 + q * 16 + x] = (quad == q) & (cell < x)
    return jnp.asarray(rows, BF16), jnp.asarray(lanes, BF16)


def pieces(value):
    first = value.astype(BF16).astype(F32)
    rest = value - first
    second = rest.astype(BF16).astype(F32)
    return first, second, rest - second


def dot(a, b, dims=((1,), (0,))):
    return lax.dot_general(a, b, (dims, ((), ())), preferred_element_type=F32)


def prep_kernel(data, mrows, mlanes, t_out, rank_out, list_out, feat0, feat1, sorted_s, t_s, meta_v, meta_s, sem):
    y, x, z, m = data[0], data[1], data[2], data[3]
    valid = m > 0.0
    one = jnp.float32(1.0)
    nil = jnp.float32(0.0)
    code = jnp.where(y >= 0.5, 4.0, 0.0) + jnp.where(z >= 0.5, 2.0, 0.0) + jnp.where(x >= 0.5, 1.0, 0.0)
    code = jnp.where(valid, code, 9.0)
    masks = [jnp.where(code == float(b), one, nil) for b in range(8)]
    stacked = jnp.concatenate(masks, 0).astype(BF16)
    row_i = lax.broadcasted_iota(jnp.int32, (PS, PS), 0)
    lane_i = lax.broadcasted_iota(jnp.int32, (PS, PS), 1)
    upper = jnp.where(row_i <= lane_i, one, nil).astype(BF16)
    running = dot(stacked, upper)
    total = dot(stacked, jnp.ones((PS, 128), BF16))
    begin = jnp.zeros((16, 128), F32)
    rank = jnp.zeros((16, PS), F32)
    for b in range(8):
        wide = jnp.concatenate([begin, begin], 1)
        rank = rank + masks[b] * (wide + running[b * 16 : b * 16 + 16] - 1.0)
        begin = begin + total[b * 16 : b * 16 + 16]
    rank = jnp.where(valid, rank, -1.0)
    rank_out[...] = rank

    columns = dot(mrows[...], total.astype(BF16))
    base = [jnp.zeros((1, 128), F32)]
    for q in range(3):
        end = base[q] + columns[192 + q : 193 + q] + float(GAP + 15)
        base.append(jnp.floor(end * 0.0625) * 16.0)
    base_col = jnp.concatenate([jnp.broadcast_to(b, (RC, 128)) for b in base], 0)
    low, high = columns[0:96], columns[96:192]
    first = jnp.floor((low + base_col) * 0.0625) * 16.0
    n_blocks = jnp.floor((high + base_col - first + float(BLOCK - 1)) * (1.0 / BLOCK))
    n_blocks = jnp.where(high > low, n_blocks, 0.0)
    gi = lax.broadcasted_iota(jnp.int32, (96, 96), 0)
    gj = lax.broadcasted_iota(jnp.int32, (96, 96), 1)
    before = dot(jnp.where(gj < gi, one, nil).astype(BF16), n_blocks.astype(BF16))
    g128 = lax.broadcasted_iota(jnp.int32, (RC, 128), 0)
    tag = jnp.concatenate([(g128 + 32 * q).astype(F32) for q in range(4)], 0)
    null = float(NULL_ROW * 128 + 23)
    lane96 = lax.broadcasted_iota(jnp.int32, (96, 128), 1).astype(F32)
    out_rows = []
    for t in range(4):
        away = lane96 + float(128 * t) - before
        inside = (away >= 0.0) & (away < n_blocks)
        entry = (first + away * float(BLOCK)) * 128.0 + tag - null
        out_rows.append(jnp.sum(jnp.where(inside, entry, 0.0), 0, keepdims=True) + null)
    out_rows.append(before[95:96] + n_blocks[95:96])
    total_row = dot(jnp.ones((8, PS), BF16), stacked, ((1,), (1,)))
    meta = dot(total_row.astype(BF16), mlanes[...])
    lane1 = lax.broadcasted_iota(jnp.int32, (1, 128), 1)
    base_lane = jnp.where(lane1 < 16, base[0], jnp.where(lane1 < 32, base[1], jnp.where(lane1 < 48, base[2], base[3])))
    out_rows.append(meta[0:1, 0:128])
    out_rows.append(meta[0:1, 128:256] + base_lane)
    longest = jnp.where(lane1 >= 64, meta[0:1, 0:128], 0.0)
    flags = jnp.zeros((1, 128), F32)
    for q in range(4):
        top = jnp.max(jnp.where((lane1 >= 64 + 16 * q) & (lane1 < 80 + 16 * q), longest, 0.0), 1, keepdims=True)
        flags = jnp.where(lane1 == q, top, flags)
    out_rows.append(flags)
    table = jnp.concatenate(out_rows, 0).astype(jnp.int32)
    list_out[...] = table
    meta_v[...] = table
    copy = pltpu.make_async_copy(meta_v, meta_s, sem)
    copy.start()

    cell_i = lax.broadcasted_iota(jnp.int32, (16, PS), 0).astype(F32)
    xg = x + (cell_i - 8.0)
    norm = y * y + xg * xg + z * z
    py, pz, px, pn = pieces(y), pieces(z), pieces(xg), pieces(norm)
    features = [py[a] for a, _ in SHORT] + [pz[a] for a, _ in SHORT] + [px[a] for a, _ in FULL] + [pn[a] for a, _ in FULL]
    ones = jnp.ones((16, PS), F32)
    features = features + [ones, ones, ones, jnp.zeros((16, PS), F32)]
    for k in range(KD):
        feat0[pl.ds(k, 16, stride=STRIDE), :] = features[k][:, 0:128]
        feat1[pl.ds(k, 16, stride=STRIDE), :] = features[k][:, 128:256]
    t_s[...] = jnp.zeros(t_s.shape, F32)
    row_b = row_i.astype(F32).astype(BF16)
    for c in range(16):
        place = jnp.where(row_b == rank[c : c + 1].astype(BF16), jnp.bfloat16(1.0), jnp.bfloat16(0.0))
        both = jnp.concatenate([feat0[c * STRIDE : c * STRIDE + KD, :], feat1[c * STRIDE : c * STRIDE + KD, :]], 1)
        sorted_s[c, 0:PS, :] = dot(place, both.astype(BF16), ((1,), (1,)))
        sorted_s[c, PS : PS + MOVE, :] = jnp.zeros((MOVE, KD), F32)
    copy.wait()
    for q in range(4):

        def place_of(c, q=q):
            return meta_s[5, q * 16 + c], meta_s[5, 64 + q * 16 + c], meta_s[6, q * 16 + c]

        @pl.when(meta_s[7, q] <= MOVE)
        def _():
            for c in range(16):
                source, _, target = place_of(c)
                t_s[pl.ds(target, MOVE), :] = sorted_s[c, pl.ds(source, MOVE), :]

        @pl.when(meta_s[7, q] > MOVE)
        def _():
            def append(c, carry):
                source, count, target = place_of(c)

                def chunk(i, carry):
                    t_s[pl.ds(target + 64 * i, 64), :] = sorted_s[c, pl.ds(source + 64 * i, 64), :]
                    return carry

                return lax.fori_loop(0, (count + 63) // 64, chunk, carry)

            lax.fori_loop(0, 16, append, 0)

    t_out[...] = t_s[...].astype(BF16)


def pair_kernel(pencils, first_of, second_of, n_in, last, *refs):
    table, shift = refs[0], refs[1]
    inputs = refs[2 : 2 + n_in]
    targets = refs[2 + n_in]
    refs = refs[3 + n_in :]
    if last:
        rank_ref, _, _, out, acc1, acc2 = refs[:6]
        back, refs = refs[6], refs[7:]
        back[...] = jnp.zeros(back.shape, F32)
    else:
        acc1, acc2 = refs[:2]
        refs = refs[2:]
        acc1[...] = jnp.zeros(acc1.shape, F32)
        acc2[...] = jnp.zeros(acc2.shape, F32)
    roll_s, stage0, stage1, weights, c_lo, c_hi, d_a, d_b = refs
    row_i = lax.broadcasted_iota(jnp.int32, (RC, PS), 0).astype(F32)
    for p, (which, index, dy, dz) in enumerate(pencils):
        start = 15 if dy == 0 else lax.rem(shift[0 if dy < 0 else 1] + 15, 16)
        rolled = []
        for f in range(4):
            value = inputs[which][index, f]
            for half in range(2):
                part = value[:, half * 128 : half * 128 + 128]
                for copy in range(3):
                    roll_s[p, 2 * f + half, copy * 16 : copy * 16 + 16, :] = part
            rolled.append(
                jnp.concatenate([roll_s[p, 2 * f, pl.ds(start, RC), :], roll_s[p, 2 * f + 1, pl.ds(start, RC), :]], 1)
            )
        y, x, z, m = rolled
        y = y + float(dy)
        z = z + float(dz)
        x = x + (row_i - 9.0)
        live = (m > 0.0) & (row_i < 18.0)
        cube = jnp.where(live, m, 1.0) * (16.0 / 3.141592653589793)
        c = jnp.where(live, jnp.exp2(jnp.log2(cube) * (1.0 / 3.0)), 0.0)
        w = c * c * 16.0
        norm = w * (y * y + x * x + z * z)
        w2 = w * -2.0
        py, pz, px, pw, pn = pieces(y * w2), pieces(z * w2), pieces(x * w2), pieces(w), pieces(norm)
        features = [py[b] for _, b in SHORT] + [pz[b] for _, b in SHORT] + [px[b] for _, b in FULL] + [pw[b] for _, b in FULL]
        features = features + list(pn) + [jnp.zeros((RC, PS), F32)]
        for k in range(KD):
            stage0[p, pl.ds(k, RC, stride=STRIDE), :] = features[k][:, 0:128]
            stage1[p, pl.ds(k, RC, stride=STRIDE), :] = features[k][:, 128:256]
        c_lo[pl.ds(p * RC, RC), :] = c[:, 0:128]
        c_hi[pl.ds(p * RC, RC), :] = c[:, 128:256]
        for r in range(RC):
            if r < 18 or r == 23:
                weights[p * RC + r, :, 0:128] = stage0[p, r * STRIDE : r * STRIDE + KD, :].astype(BF16)
                weights[p * RC + r, :, 128:256] = stage1[p, r * STRIDE : r * STRIDE + KD, :].astype(BF16)

    def decode(i):
        entry = table[lax.shift_right_logical(i, 7), lax.bitwise_and(i, 127)]
        at = pl.multiple_of(lax.shift_left(lax.shift_right_logical(entry, 11), 4), 16)
        q = lax.bitwise_and(lax.shift_right_logical(entry, 5), 3)
        r = lax.bitwise_and(entry, 31)
        return at, first_of(q) * RC + r, second_of(q) * RC + r

    def multiply(i, slot):
        at, w_a, w_b = decode(i)
        lhs = targets[pl.ds(at, BLOCK), :]
        slot[:, 0:256] = dot(lhs, weights[w_a])
        slot[:, 256:512] = dot(lhs, weights[w_b])

    def consume(i, slot):
        at, w_a, w_b = decode(i)
        cs = []
        for ref, w in ((c_lo, w_a), (c_hi, w_a), (c_lo, w_b), (c_hi, w_b)):
            cs.append(ref[pl.ds(w, 8, stride=0), :])
        for g in range(BLOCK // 8):
            sum1 = acc1[pl.ds(at + 8 * g, 8), :]
            sum2 = acc2[pl.ds(at + 8 * g, 8), :]
            for t in range(4):
                square = jnp.maximum(slot[8 * g : 8 * g + 8, 128 * t : 128 * t + 128], 1e-30)
                root = square * lax.rsqrt(square)
                inner = cs[t] - root
                outer = jnp.maximum(inner + cs[t], 0.0)
                inner = jnp.maximum(inner, 0.0)
                sum1 = sum1 + outer * outer * outer
                sum2 = sum2 + inner * inner * inner
            acc1[pl.ds(at + 8 * g, 8), :] = sum1
            acc2[pl.ds(at + 8 * g, 8), :] = sum2

    count = table[4, 0]
    for k in range(GROUP // 2):
        multiply(k, d_a.at[k])

    def step(it, carry):
        i = it * GROUP
        half = GROUP // 2
        for k in range(half):
            multiply(i + half + k, d_b.at[k])
        for k in range(half):
            consume(i + k, d_a.at[k])
        for k in range(half):
            multiply(i + GROUP + k, d_a.at[k])
        for k in range(half):
            consume(i + half + k, d_b.at[k])
        return carry

    lax.fori_loop(0, (count + GROUP - 1) // GROUP, step, 0)

    if last:
        unsort(table, acc1, acc2, back, rank_ref, out)


def unsort(table, acc1, acc2, back, rank_ref, out):
    for q in range(4):

        def place_of(c, q=q):
            return table[5, q * 16 + c], table[5, 64 + q * 16 + c], table[6, q * 16 + c]

        @pl.when(table[7, q] <= MOVE)
        def _():
            for c in range(16):
                target, _, source = place_of(c)
                value = acc1[pl.ds(source, MOVE), :] - 4.0 * acc2[pl.ds(source, MOVE), :]
                back[c, pl.ds(target, MOVE), :] = value

        @pl.when(table[7, q] > MOVE)
        def _():
            def fetch(c, carry):
                target, length, source = place_of(c)

                def chunk(i, carry):
                    value = acc1[pl.ds(source + 64 * i, 64), :] - 4.0 * acc2[pl.ds(source + 64 * i, 64), :]
                    back[c, pl.ds(target + 64 * i, 64), :] = value
                    return carry

                return lax.fori_loop(0, (length + 63) // 64, chunk, carry)

            lax.fori_loop(0, 16, fetch, 0)

    row_b = lax.broadcasted_iota(jnp.int32, (PS, PS), 0).astype(F32).astype(BF16)
    row8 = lax.broadcasted_iota(jnp.int32, (8, PS), 0)
    ones = jnp.ones((8, 128), BF16)
    for c in range(16):
        value = back[c, 0:PS, :]
        high = value.astype(BF16)
        low = (value - high.astype(F32)).astype(BF16)
        sums = dot(ones, high, ((1,), (1,))) + dot(ones, low, ((1,), (1,)))
        s1, s2, s3 = pieces(sums)
        lhs = jnp.where(row8 == 0, s1, jnp.where(row8 == 1, s2, jnp.where(row8 == 2, s3, 0.0))).astype(BF16)
        place = jnp.where(row_b == rank_ref[c : c + 1, :].astype(BF16), jnp.bfloat16(1.0), jnp.bfloat16(0.0))
        out[c : c + 1, :] = jnp.sum(dot(lhs, place), 0, keepdims=True)


VMEM_SPEC = pl.BlockSpec(memory_space=pltpu.VMEM)
SMEM_SPEC = pl.BlockSpec(memory_space=pltpu.SMEM)


def prepare(data, interpret=False):
    mrows, mlanes = constants()
    return pl.pallas_call(
        prep_kernel,
        out_shape=(
            jax.ShapeDtypeStruct((ROWS, KD), BF16),
            jax.ShapeDtypeStruct((NX, PS), F32),
            jax.ShapeDtypeStruct((8, 128), jnp.int32),
        ),
        in_specs=[VMEM_SPEC] * 3,
        out_specs=[VMEM_SPEC] * 3,
        scratch_shapes=[
            pltpu.VMEM((16 * STRIDE, 128), F32),
            pltpu.VMEM((16 * STRIDE, 128), F32),
            pltpu.VMEM((16, PS + MOVE, KD), F32),
            pltpu.VMEM((ROWS, KD), F32),
            pltpu.VMEM((8, 128), jnp.int32),
            pltpu.SMEM((8, 128), jnp.int32),
            pltpu.SemaphoreType.DMA,
        ],
        compiler_params=pltpu.CompilerParams(vmem_limit_bytes=40 << 20),
        interpret=interpret,
        name="prepare",
    )(data, mrows, mlanes)


def pair_sums(pencils, first_of, second_of, table, shift, inputs, targets, rest, name, interpret=False):
    n = len(pencils)
    last = len(rest) > 0
    sums = [jax.ShapeDtypeStruct((ROWS, 128), F32)] * 2
    out_shape = [jax.ShapeDtypeStruct((NX, PS), F32)] + sums if last else sums
    at = len(inputs) + 4
    scratch = [
        pltpu.VMEM((n, 8, 48, 128), F32),
        pltpu.VMEM((n, RC * STRIDE, 128), F32),
        pltpu.VMEM((n, RC * STRIDE, 128), F32),
        pltpu.VMEM((n * RC, KD, PS), BF16),
        pltpu.VMEM((n * RC, 128), F32),
        pltpu.VMEM((n * RC, 128), F32),
        pltpu.VMEM((GROUP // 2, BLOCK, 512), F32),
        pltpu.VMEM((GROUP // 2, BLOCK, 512), F32),
    ]
    if last:
        scratch = [pltpu.VMEM((NX, PS + MOVE, 128), F32)] + scratch
    return pl.pallas_call(
        functools.partial(pair_kernel, pencils, first_of, second_of, len(inputs), last),
        out_shape=out_shape,
        in_specs=[SMEM_SPEC] * 2 + [VMEM_SPEC] * (len(inputs) + 1 + len(rest)),
        out_specs=[VMEM_SPEC] * len(out_shape),
        scratch_shapes=scratch,
        input_output_aliases={at: 1, at + 1: 2} if last else {},
        compiler_params=pltpu.CompilerParams(vmem_limit_bytes=40 << 20),
        interpret=interpret,
        name=name,
    )(table, shift, *inputs, targets, *rest)


PENCILS_A = ((0, 0, 0, 0), (0, 1, -1, 0), (0, 2, 1, 0))
PENCILS_B = ((0, 0, 0, -1), (1, 0, 0, 1), (0, 1, -1, -1), (1, 1, -1, 1), (0, 2, 1, -1), (1, 2, 1, 1))


def near_sums(table, shift, rows, targets, interpret=False):
    return pair_sums(
        PENCILS_A, lambda q: 0, lambda q: 1 + lax.shift_right_logical(q, 1), table, shift, [rows], targets, [], "near", interpret
    )


def far_sums(table, shift, low, high, targets, rank, sums, interpret=False):
    return pair_sums(
        PENCILS_B, lambda q: lax.bitwise_and(q, 1), lambda q: 2 + q, table, shift, [low, high], targets, [rank, *sums], "far", interpret
    )[0]


def ring(axis, distance):
    count = lax.axis_size(axis)
    return [(i, (i + distance) % count) for i in range(count)]


def shards(positions, masses, counts, shear_offset):
    slot_index = lax.broadcasted_iota(jnp.int32, masses.shape, 3)
    weight = jnp.where(slot_index < counts[..., None], masses, jnp.float32(0.0))
    data = jnp.concatenate([positions, weight[None]], 0).reshape(4, NX, PS)
    index = lax.axis_index("shear")
    offset = shear_offset[0]
    shift = jnp.stack([
        jnp.where(index == 0, NX - offset, 0),
        jnp.where(index == lax.axis_size("shear") - 1, offset, 0),
    ]).astype(jnp.int32)
    below = lax.ppermute(data, "shear", ring("shear", 1))
    above = lax.ppermute(data, "shear", ring("shear", -1))
    targets, rank, table = prepare(data)
    rows = jnp.stack([data, below, above])
    rows, targets, rank, table = lax.optimization_barrier((rows, targets, rank, table))
    low = lax.ppermute(rows, "cross", ring("cross", 1))
    high = lax.ppermute(rows, "cross", ring("cross", -1))
    sums = near_sums(table, shift, rows, targets)
    density = far_sums(table, shift, low, high, targets, rank, sums)
    return density.reshape(masses.shape)


def solution(mesh):
    in_specs = (
        P(None, "shear", None, "cross", None),
        P("shear", None, "cross", None),
        P("shear", None, "cross"),
        P(),
    )
    out_specs = P("shear", None, "cross", None)
    return jax.shard_map(shards, mesh=mesh, in_specs=in_specs, out_specs=out_specs, check_vma=False)
```

```python
import functools

import jax
import jax.numpy as jnp
import numpy as np
from jax import lax
from jax.experimental import pallas as pl
from jax.experimental.pallas import tpu as pltpu
from jax.sharding import PartitionSpec as P

NX = 16
PS = 256
ROWS = 4480
NULL_ROW = 4416
BLOCK = 32
GROUP = 8
GAP = 48
MOVE = 96
RC = 24
STRIDE = 33
KD = 32
ITEMS = 512
META = 5 * ITEMS
F32 = jnp.float32
BF16 = jnp.bfloat16

FULL = [(0, 0), (0, 1), (0, 2), (1, 0), (1, 1), (1, 2), (2, 0), (2, 1)]
SHORT = [(0, 0), (0, 1), (0, 2), (1, 0), (1, 1), (2, 0)]


def constants():
    j = np.arange(128)
    bins, cell = j // 16, j % 16
    quad, half = bins // 2, bins % 2
    place = 2 * cell + half
    rows = np.zeros((200, 128), np.float32)
    for q in range(4):
        for r in range(18):
            low, high = max(2 * (r - 1) - 1, 0), min(2 * (r - 1) + 3, 32)
            rows[q * RC + r] = (quad == q) & (place < low)
            rows[96 + q * RC + r] = (quad == q) & (place < high)
        rows[192 + q] = quad == q
    lanes = np.zeros((128, 256), np.float32)
    for q in range(4):
        for x in range(16):
            lanes[:, q * 16 + x] = (cell == x) & (quad < q)
            lanes[:, 64 + q * 16 + x] = (cell == x) & (quad == q)
            lanes[:, 128 + q * 16 + x] = (quad == q) & (cell < x)
    return jnp.asarray(rows, BF16), jnp.asarray(lanes, BF16)


def pieces(value):
    first = value.astype(BF16).astype(F32)
    rest = value - first
    second = rest.astype(BF16).astype(F32)
    return first, second, rest - second


def dot(a, b, dims=((1,), (0,))):
    return lax.dot_general(a, b, (dims, ((), ())), preferred_element_type=F32)


def prep_kernel(data, mrows, mlanes, t_out, rank_out, list_out, feat0, feat1, sorted_s, t_s, meta_v, meta_s, sem):
    y, x, z, m = data[0], data[1], data[2], data[3]
    valid = m > 0.0
    one = jnp.float32(1.0)
    nil = jnp.float32(0.0)
    code = jnp.where(y >= 0.5, 4.0, 0.0) + jnp.where(z >= 0.5, 2.0, 0.0) + jnp.where(x >= 0.5, 1.0, 0.0)
    code = jnp.where(valid, code, 9.0)
    masks = [jnp.where(code == float(b), one, nil) for b in range(8)]
    stacked = jnp.concatenate(masks, 0).astype(BF16)
    row_i = lax.broadcasted_iota(jnp.int32, (PS, PS), 0)
    lane_i = lax.broadcasted_iota(jnp.int32, (PS, PS), 1)
    upper = jnp.where(row_i <= lane_i, one, nil).astype(BF16)
    running = dot(stacked, upper)
    total = dot(stacked, jnp.ones((PS, 128), BF16))
    begin = jnp.zeros((16, 128), F32)
    rank = jnp.zeros((16, PS), F32)
    for b in range(8):
        wide = jnp.concatenate([begin, begin], 1)
        rank = rank + masks[b] * (wide + running[b * 16 : b * 16 + 16] - 1.0)
        begin = begin + total[b * 16 : b * 16 + 16]
    rank = jnp.where(valid, rank, -1.0)
    rank_out[...] = rank

    columns = dot(mrows[...], total.astype(BF16))
    base = [jnp.zeros((1, 128), F32)]
    for q in range(3):
        end = base[q] + columns[192 + q : 193 + q] + float(GAP + 15)
        base.append(jnp.floor(end * 0.0625) * 16.0)
    base_col = jnp.concatenate([jnp.broadcast_to(b, (RC, 128)) for b in base], 0)
    low, high = columns[0:96], columns[96:192]
    first = jnp.floor((low + base_col) * 0.0625) * 16.0
    n_blocks = jnp.floor((high + base_col - first + float(BLOCK - 1)) * (1.0 / BLOCK))
    n_blocks = jnp.where(high > low, n_blocks, 0.0)
    gi = lax.broadcasted_iota(jnp.int32, (96, 96), 0)
    gj = lax.broadcasted_iota(jnp.int32, (96, 96), 1)
    before = dot(jnp.where(gj < gi, one, nil).astype(BF16), n_blocks.astype(BF16))
    group_r = lax.broadcasted_iota(jnp.int32, (96, 128), 0)
    group_q = group_r // RC
    cell_r = group_r - group_q * RC
    fields = [
        cell_r,
        cell_r + RC * (1 + group_q // 2),
        cell_r + RC * lax.bitwise_and(group_q, 1),
        cell_r + RC * (2 + group_q),
    ]
    lane96 = lax.broadcasted_iota(jnp.int32, (96, 128), 1).astype(F32)
    away = [lane96 + float(128 * t) - before for t in range(4)]
    inside = [(v >= 0.0) & (v < n_blocks) for v in away]
    out_rows = []
    for t in range(4):
        entry = first + away[t] * float(BLOCK) - float(NULL_ROW)
        out_rows.append(jnp.sum(jnp.where(inside[t], entry, 0.0), 0, keepdims=True) + float(NULL_ROW))
    for field in fields:
        entry = field.astype(F32) - float(RC - 1)
        for t in range(4):
            out_rows.append(jnp.sum(jnp.where(inside[t], entry, 0.0), 0, keepdims=True) + float(RC - 1))
    out_rows.append(before[95:96] + n_blocks[95:96])
    total_row = dot(jnp.ones((8, PS), BF16), stacked, ((1,), (1,)))
    meta = dot(total_row.astype(BF16), mlanes[...])
    lane1 = lax.broadcasted_iota(jnp.int32, (1, 128), 1)
    base_lane = jnp.where(lane1 < 16, base[0], jnp.where(lane1 < 32, base[1], jnp.where(lane1 < 48, base[2], base[3])))
    out_rows.append(meta[0:1, 0:128])
    out_rows.append(meta[0:1, 128:256] + base_lane)
    longest = jnp.where(lane1 >= 64, meta[0:1, 0:128], 0.0)
    flags = jnp.zeros((1, 128), F32)
    for q in range(4):
        top = jnp.max(jnp.where((lane1 >= 64 + 16 * q) & (lane1 < 80 + 16 * q), longest, 0.0), 1, keepdims=True)
        flags = jnp.where(lane1 == q, top, flags)
    out_rows.append(flags)
    table = jnp.concatenate(out_rows, 0).astype(jnp.int32)
    list_out[...] = table
    meta_v[...] = table
    copy = pltpu.make_async_copy(meta_v, meta_s, sem)
    copy.start()

    cell_i = lax.broadcasted_iota(jnp.int32, (16, PS), 0).astype(F32)
    xg = x + (cell_i - 8.0)
    norm = y * y + xg * xg + z * z
    py, pz, px, pn = pieces(y), pieces(z), pieces(xg), pieces(norm)
    features = [py[a] for a, _ in SHORT] + [pz[a] for a, _ in SHORT] + [px[a] for a, _ in FULL] + [pn[a] for a, _ in FULL]
    ones = jnp.ones((16, PS), F32)
    features = features + [ones, ones, ones, jnp.zeros((16, PS), F32)]
    for k in range(KD):
        feat0[pl.ds(k, 16, stride=STRIDE), :] = features[k][:, 0:128]
        feat1[pl.ds(k, 16, stride=STRIDE), :] = features[k][:, 128:256]
    t_s[...] = jnp.zeros(t_s.shape, F32)
    row_b = row_i.astype(F32).astype(BF16)
    for c in range(16):
        place = jnp.where(row_b == rank[c : c + 1].astype(BF16), jnp.bfloat16(1.0), jnp.bfloat16(0.0))
        both = jnp.concatenate([feat0[c * STRIDE : c * STRIDE + KD, :], feat1[c * STRIDE : c * STRIDE + KD, :]], 1)
        sorted_s[c, 0:PS, :] = dot(place, both.astype(BF16), ((1,), (1,)))
        sorted_s[c, PS : PS + MOVE, :] = jnp.zeros((MOVE, KD), F32)
    copy.wait()
    for q in range(4):

        def place_of(c, q=q):
            return meta_s[21, q * 16 + c], meta_s[21, 64 + q * 16 + c], meta_s[22, q * 16 + c]

        @pl.when(meta_s[23, q] <= MOVE)
        def _():
            for c in range(16):
                source, _, target = place_of(c)
                t_s[pl.ds(target, MOVE), :] = sorted_s[c, pl.ds(source, MOVE), :]

        @pl.when(meta_s[23, q] > MOVE)
        def _():
            def append(c, carry):
                source, count, target = place_of(c)

                def chunk(i, carry):
                    t_s[pl.ds(target + 64 * i, 64), :] = sorted_s[c, pl.ds(source + 64 * i, 64), :]
                    return carry

                return lax.fori_loop(0, (count + 63) // 64, chunk, carry)

            lax.fori_loop(0, 16, append, 0)

    t_out[...] = t_s[...].astype(BF16)


def pair_kernel(pencils, first_of, n_in, last, *refs):
    table, shift = refs[0], refs[1]
    inputs = refs[2 : 2 + n_in]
    targets = refs[2 + n_in]
    refs = refs[3 + n_in :]
    if last:
        rank_ref, _, _, out, acc1, acc2 = refs[:6]
        back, refs = refs[6], refs[7:]
    else:
        acc1, acc2 = refs[:2]
        refs = refs[2:]
        acc1[...] = jnp.zeros(acc1.shape, F32)
        acc2[...] = jnp.zeros(acc2.shape, F32)
    roll_s, stage0, stage1, weights, c_lo, c_hi, squares = refs
    row_i = lax.broadcasted_iota(jnp.int32, (RC, PS), 0).astype(F32)
    for p, (which, index, dy, dz) in enumerate(pencils):
        start = 15 if dy == 0 else lax.rem(shift[0 if dy < 0 else 1] + 15, 16)
        rolled = []
        for f in range(4):
            value = inputs[which][index, f]
            for half in range(2):
                part = value[:, half * 128 : half * 128 + 128]
                for copy in range(3):
                    roll_s[p, 2 * f + half, copy * 16 : copy * 16 + 16, :] = part
            rolled.append(
                jnp.concatenate([roll_s[p, 2 * f, pl.ds(start, RC), :], roll_s[p, 2 * f + 1, pl.ds(start, RC), :]], 1)
            )
        y, x, z, m = rolled
        y = y + float(dy)
        z = z + float(dz)
        x = x + (row_i - 9.0)
        live = (m > 0.0) & (row_i < 18.0)
        cube = jnp.where(live, m, 1.0) * (16.0 / 3.141592653589793)
        c = jnp.where(live, jnp.exp2(jnp.log2(cube) * (1.0 / 3.0)), 0.0)
        w = c * c * 16.0
        norm = w * (y * y + x * x + z * z)
        w2 = w * -2.0
        py, pz, px, pw, pn = pieces(y * w2), pieces(z * w2), pieces(x * w2), pieces(w), pieces(norm)
        features = [py[b] for _, b in SHORT] + [pz[b] for _, b in SHORT] + [px[b] for _, b in FULL] + [pw[b] for _, b in FULL]
        features = features + list(pn) + [jnp.zeros((RC, PS), F32)]
        for k in range(KD):
            stage0[p, pl.ds(k, RC, stride=STRIDE), :] = features[k][:, 0:128]
            stage1[p, pl.ds(k, RC, stride=STRIDE), :] = features[k][:, 128:256]
        c_lo[pl.ds(p * RC, RC), :] = c[:, 0:128]
        c_hi[pl.ds(p * RC, RC), :] = c[:, 128:256]
        for r in range(RC):
            if r < 18 or r == 23:
                weights[p * RC + r, :, 0:128] = stage0[p, r * STRIDE : r * STRIDE + KD, :].astype(BF16)
                weights[p * RC + r, :, 128:256] = stage1[p, r * STRIDE : r * STRIDE + KD, :].astype(BF16)

    def decode(i):
        return pl.multiple_of(table[i], 16), table[i + first_of], table[i + first_of + ITEMS]

    def multiply(i, slot):
        at, w_a, w_b = decode(i)
        lhs = targets[pl.ds(at, BLOCK), :]
        slot[:, 0:256] = dot(lhs, weights[w_a])
        slot[:, 256:512] = dot(lhs, weights[w_b])

    def consume(i, slot):
        at, w_a, w_b = decode(i)
        cs = []
        for ref, w in ((c_lo, w_a), (c_hi, w_a), (c_lo, w_b), (c_hi, w_b)):
            cs.append(ref[pl.ds(w, 8, stride=0), :])
        for g in range(BLOCK // 8):
            sum1 = acc1[pl.ds(at + 8 * g, 8), :]
            sum2 = acc2[pl.ds(at + 8 * g, 8), :]
            for t in range(4):
                square = jnp.maximum(slot[8 * g : 8 * g + 8, 128 * t : 128 * t + 128], 1e-30)
                root = square * lax.rsqrt(square)
                inner = cs[t] - root
                outer = jnp.maximum(inner + cs[t], 0.0)
                inner = jnp.maximum(inner, 0.0)
                sum1 = sum1 + outer * outer * outer
                sum2 = sum2 + inner * inner * inner
            acc1[pl.ds(at + 8 * g, 8), :] = sum1
            acc2[pl.ds(at + 8 * g, 8), :] = sum2

    count = table[META]
    for k in range(GROUP):
        multiply(k, squares.at[k])

    def step(it, carry):
        i = it * GROUP
        for k in range(GROUP):
            consume(i + k, squares.at[k])
        for k in range(GROUP):
            multiply(i + GROUP + k, squares.at[k])
        return carry

    lax.fori_loop(0, (count + GROUP - 1) // GROUP, step, 0)

    if last:
        unsort(table, acc1, acc2, back, rank_ref, out)


def unsort(table, acc1, acc2, back, rank_ref, out):
    for q in range(4):

        def place_of(c, q=q):
            at = META + 128 + q * 16 + c
            return table[at], table[at + 64], table[at + 128]

        @pl.when(table[META + 384 + q] <= MOVE)
        def _():
            for c in range(16):
                target, _, source = place_of(c)
                value = acc1[pl.ds(source, MOVE), :] - 4.0 * acc2[pl.ds(source, MOVE), :]
                back[c, pl.ds(target, MOVE), :] = value

        @pl.when(table[META + 384 + q] > MOVE)
        def _():
            def fetch(c, carry):
                target, length, source = place_of(c)

                def chunk(i, carry):
                    value = acc1[pl.ds(source + 64 * i, 64), :] - 4.0 * acc2[pl.ds(source + 64 * i, 64), :]
                    back[c, pl.ds(target + 64 * i, 64), :] = value
                    return carry

                return lax.fori_loop(0, (length + 63) // 64, chunk, carry)

            lax.fori_loop(0, 16, fetch, 0)

    row_f = lax.broadcasted_iota(jnp.int32, (PS, 128), 0).astype(F32)
    ones = jnp.ones((256, 128), BF16)
    for c in range(16):
        value = back[c, 0:PS, :]
        high = value.astype(BF16)
        low = (value - high.astype(F32)).astype(BF16)
        sums = dot(jnp.concatenate([high, low], 1), ones)
        for half in range(2):
            lanes = slice(128 * half, 128 * half + 128)
            mine = row_f == rank_ref[c : c + 1, lanes]
            out[c : c + 1, lanes] = jnp.sum(jnp.where(mine, sums, 0.0), 0, keepdims=True)


VMEM_SPEC = pl.BlockSpec(memory_space=pltpu.VMEM)
SMEM_SPEC = pl.BlockSpec(memory_space=pltpu.SMEM)


def prepare(data, interpret=False):
    mrows, mlanes = constants()
    return pl.pallas_call(
        prep_kernel,
        out_shape=(
            jax.ShapeDtypeStruct((ROWS, KD), BF16),
            jax.ShapeDtypeStruct((NX, PS), F32),
            jax.ShapeDtypeStruct((24, 128), jnp.int32),
        ),
        in_specs=[VMEM_SPEC] * 3,
        out_specs=[VMEM_SPEC] * 3,
        scratch_shapes=[
            pltpu.VMEM((16 * STRIDE, 128), F32),
            pltpu.VMEM((16 * STRIDE, 128), F32),
            pltpu.VMEM((16, PS + MOVE, KD), F32),
            pltpu.VMEM((ROWS, KD), F32),
            pltpu.VMEM((24, 128), jnp.int32),
            pltpu.SMEM((24, 128), jnp.int32),
            pltpu.SemaphoreType.DMA,
        ],
        compiler_params=pltpu.CompilerParams(vmem_limit_bytes=40 << 20),
        interpret=interpret,
        name="prepare",
    )(data, mrows, mlanes)


def pair_sums(pencils, first_of, table, shift, inputs, targets, rest, name, interpret=False):
    n = len(pencils)
    last = len(rest) > 0
    sums = [jax.ShapeDtypeStruct((ROWS, 128), F32)] * 2
    out_shape = [jax.ShapeDtypeStruct((NX, PS), F32)] + sums if last else sums
    at = len(inputs) + 4
    scratch = [
        pltpu.VMEM((n, 8, 48, 128), F32),
        pltpu.VMEM((n, RC * STRIDE, 128), F32),
        pltpu.VMEM((n, RC * STRIDE, 128), F32),
        pltpu.VMEM((n * RC, KD, PS), BF16),
        pltpu.VMEM((n * RC, 128), F32),
        pltpu.VMEM((n * RC, 128), F32),
        pltpu.VMEM((GROUP, BLOCK, 512), F32),
    ]
    if last:
        scratch = [pltpu.VMEM((NX, PS + MOVE, 128), F32)] + scratch
    return pl.pallas_call(
        functools.partial(pair_kernel, pencils, first_of, len(inputs), last),
        out_shape=out_shape,
        in_specs=[SMEM_SPEC] * 2 + [VMEM_SPEC] * (len(inputs) + 1 + len(rest)),
        out_specs=[VMEM_SPEC] * len(out_shape),
        scratch_shapes=scratch,
        input_output_aliases={at: 1, at + 1: 2} if last else {},
        compiler_params=pltpu.CompilerParams(vmem_limit_bytes=40 << 20),
        interpret=interpret,
        name=name,
    )(table, shift, *inputs, targets, *rest)


PENCILS_A = ((0, 0, 0, 0), (0, 1, -1, 0), (0, 2, 1, 0))
PENCILS_B = ((0, 0, 0, -1), (1, 0, 0, 1), (0, 1, -1, -1), (1, 1, -1, 1), (0, 2, 1, -1), (1, 2, 1, 1))


def near_sums(table, shift, rows, targets, interpret=False):
    return pair_sums(
        PENCILS_A, ITEMS, table, shift, [rows], targets, [], "near", interpret
    )


def far_sums(table, shift, low, high, targets, rank, sums, interpret=False):
    return pair_sums(
        PENCILS_B, 3 * ITEMS, table, shift, [low, high], targets, [rank, *sums], "far", interpret
    )[0]


def ring(axis, distance):
    count = lax.axis_size(axis)
    return [(i, (i + distance) % count) for i in range(count)]


def shards(positions, masses, counts, shear_offset):
    slot_index = lax.broadcasted_iota(jnp.int32, masses.shape, 3)
    weight = jnp.where(slot_index < counts[..., None], masses, jnp.float32(0.0))
    data = jnp.concatenate([positions, weight[None]], 0).reshape(4, NX, PS)
    index = lax.axis_index("shear")
    offset = shear_offset[0]
    shift = jnp.stack([
        jnp.where(index == 0, NX - offset, 0),
        jnp.where(index == lax.axis_size("shear") - 1, offset, 0),
    ]).astype(jnp.int32)
    below = lax.ppermute(data, "shear", ring("shear", 1))
    above = lax.ppermute(data, "shear", ring("shear", -1))
    targets, rank, table = prepare(data)
    table = table.reshape(-1)
    rows = jnp.stack([data, below, above])
    rows, targets, rank, table = lax.optimization_barrier((rows, targets, rank, table))
    low = lax.ppermute(rows, "cross", ring("cross", 1))
    high = lax.ppermute(rows, "cross", ring("cross", -1))
    sums = near_sums(table, shift, rows, targets)
    density = far_sums(table, shift, low, high, targets, rank, sums)
    return density.reshape(masses.shape)


def solution(mesh):
    in_specs = (
        P(None, "shear", None, "cross", None),
        P("shear", None, "cross", None),
        P("shear", None, "cross"),
        P(),
    )
    out_specs = P("shear", None, "cross", None)
    return jax.shard_map(shards, mesh=mesh, in_specs=in_specs, out_specs=out_specs, check_vma=False)
```

```python
import functools

import jax
import jax.numpy as jnp
from jax import lax
from jax.experimental import pallas as pl
from jax.experimental.pallas import tpu as pltpu
from jax.sharding import PartitionSpec as P

NX = 16
PS = 256
ROWS = 4480
NULL_ROW = 4416
BLOCK = 32
GAP = 48
MOVE = 96
RC = 24
STRIDE = 33
KD = 32
ITEMS = 512
META = 5 * ITEMS
F32 = jnp.float32
BF16 = jnp.bfloat16

FULL = [(0, 0), (0, 1), (0, 2), (1, 0), (1, 1), (1, 2), (2, 0), (2, 1)]
SHORT = [(0, 0), (0, 1), (0, 2), (1, 0), (1, 1), (2, 0)]


def pieces(value):
    first = value.astype(BF16).astype(F32)
    rest = value - first
    second = rest.astype(BF16).astype(F32)
    return first, second, rest - second


def dot(a, b, dims=((1,), (0,))):
    return lax.dot_general(a, b, (dims, ((), ())), preferred_element_type=F32)


def steps(value, width, most):
    return sum((value >= width * (i + 1)).astype(jnp.int32) for i in range(most))


def prep_kernel(data, t_out, rank_out, list_out, feat0, feat1, sorted_s, t_s, meta_v, meta_s, sem):
    y, x, z, m = data[0], data[1], data[2], data[3]
    valid = m > 0.0
    one = jnp.float32(1.0)
    nil = jnp.float32(0.0)
    code = jnp.where(y >= 0.5, 4.0, 0.0) + jnp.where(z >= 0.5, 2.0, 0.0) + jnp.where(x >= 0.5, 1.0, 0.0)
    code = jnp.where(valid, code, 9.0)
    masks = [jnp.where(code == float(b), one, nil) for b in range(8)]
    stacked = jnp.concatenate(masks, 0).astype(BF16)
    row_i = lax.broadcasted_iota(jnp.int32, (PS, PS), 0)
    lane_i = lax.broadcasted_iota(jnp.int32, (PS, PS), 1)
    upper = jnp.where(row_i <= lane_i, one, nil).astype(BF16)
    running = dot(stacked, upper)
    total = dot(stacked, jnp.ones((PS, 128), BF16))
    begin = jnp.zeros((16, 128), F32)
    rank = jnp.zeros((16, PS), F32)
    for b in range(8):
        wide = jnp.concatenate([begin, begin], 1)
        rank = rank + masks[b] * (wide + running[b * 16 : b * 16 + 16] - 1.0)
        begin = begin + total[b * 16 : b * 16 + 16]
    rank = jnp.where(valid, rank, -1.0)
    rank_out[...] = rank

    g = lax.broadcasted_iota(jnp.int32, (200, 128), 0)
    j = lax.broadcasted_iota(jnp.int32, (200, 128), 1)
    kind = steps(g, 96, 2)
    g = g - 96 * kind
    group_q = steps(g, RC, 3)
    group_x = g - RC * group_q - 1
    limit = jnp.where(kind == 0, 2 * group_x - 1, jnp.where(group_x > 16, 0, 2 * group_x + 3))
    limit = jnp.where((kind == 0) & (group_x > 16), 0, limit)
    limit = jnp.where(kind == 2, 32, limit)
    group_q = jnp.where(kind == 2, g, group_q)
    spot = 2 * (j & 15) + ((j >> 4) & 1)
    counted = ((j >> 5) == group_q) & (spot < limit)
    columns = dot(jnp.where(counted, one, nil).astype(BF16), total.astype(BF16))
    base = [jnp.zeros((1, 128), F32)]
    for q in range(3):
        end = base[q] + columns[192 + q : 193 + q] + float(GAP + 15)
        base.append(jnp.floor(end * 0.0625) * 16.0)
    base_col = jnp.concatenate([jnp.broadcast_to(b, (RC, 128)) for b in base], 0)
    low, high = columns[0:96], columns[96:192]
    first = jnp.floor((low + base_col) * 0.0625) * 16.0
    n_blocks = jnp.floor((high + base_col - first + float(BLOCK - 1)) * (1.0 / BLOCK))
    n_blocks = jnp.where(high > low, n_blocks, 0.0)
    gi = lax.broadcasted_iota(jnp.int32, (96, 96), 0)
    gj = lax.broadcasted_iota(jnp.int32, (96, 96), 1)
    before = dot(jnp.where(gj < gi, one, nil).astype(BF16), n_blocks.astype(BF16))
    group_r = lax.broadcasted_iota(jnp.int32, (96, 128), 0)
    group_q = steps(group_r, RC, 3)
    cell_r = group_r - group_q * RC
    fields = [
        cell_r,
        cell_r + RC * (group_q >> 1),
        cell_r + RC * (group_q & 1),
        cell_r + RC * (2 + group_q),
    ]
    lane96 = lax.broadcasted_iota(jnp.int32, (96, 128), 1).astype(F32)
    away = [lane96 + float(128 * t) - before for t in range(4)]
    inside = [(v >= 0.0) & (v < n_blocks) for v in away]
    out_rows = []
    for t in range(4):
        entry = first + away[t] * float(BLOCK) - float(NULL_ROW)
        out_rows.append(jnp.sum(jnp.where(inside[t], entry, 0.0), 0, keepdims=True) + float(NULL_ROW))
    for field in fields:
        entry = field.astype(F32) - float(RC - 1)
        for t in range(4):
            out_rows.append(jnp.sum(jnp.where(inside[t], entry, 0.0), 0, keepdims=True) + float(RC - 1))
    out_rows.append(before[95:96] + n_blocks[95:96])
    total_row = dot(jnp.ones((8, PS), BF16), stacked, ((1,), (1,)))
    j = lax.broadcasted_iota(jnp.int32, (128, 256), 0)
    k = lax.broadcasted_iota(jnp.int32, (128, 256), 1)
    quad, kind, goal = j >> 5, k >> 6, (k & 63) >> 4
    same, earlier = (j & 15) == (k & 15), (j & 15) < (k & 15)
    counted = ((kind == 0) & same & (quad < goal)) | ((kind == 1) & same & (quad == goal))
    counted = counted | ((kind == 2) & earlier & (quad == goal))
    meta = dot(total_row.astype(BF16), jnp.where(counted, one, nil).astype(BF16))
    lane1 = lax.broadcasted_iota(jnp.int32, (1, 128), 1)
    base_lane = jnp.where(lane1 < 16, base[0], jnp.where(lane1 < 32, base[1], jnp.where(lane1 < 48, base[2], base[3])))
    out_rows.append(meta[0:1, 0:128])
    out_rows.append(meta[0:1, 128:256] + base_lane)
    longest = jnp.where(lane1 >= 64, meta[0:1, 0:128], 0.0)
    flags = jnp.zeros((1, 128), F32)
    for q in range(4):
        top = jnp.max(jnp.where((lane1 >= 64 + 16 * q) & (lane1 < 80 + 16 * q), longest, 0.0), 1, keepdims=True)
        flags = jnp.where(lane1 == q, top, flags)
    out_rows.append(flags)
    table = jnp.concatenate(out_rows, 0).astype(jnp.int32)
    list_out[...] = table
    meta_v[...] = table
    copy = pltpu.make_async_copy(meta_v, meta_s, sem)
    copy.start()

    cell_i = lax.broadcasted_iota(jnp.int32, (16, PS), 0).astype(F32)
    xg = x + (cell_i - 8.0)
    norm = y * y + xg * xg + z * z
    py, pz, px, pn = pieces(y), pieces(z), pieces(xg), pieces(norm)
    features = [py[a] for a, _ in SHORT] + [pz[a] for a, _ in SHORT] + [px[a] for a, _ in FULL] + [pn[a] for a, _ in FULL]
    ones = jnp.ones((16, PS), F32)
    features = features + [ones, ones, ones, jnp.zeros((16, PS), F32)]
    for k in range(KD):
        feat0[pl.ds(k, 16, stride=STRIDE), :] = features[k][:, 0:128]
        feat1[pl.ds(k, 16, stride=STRIDE), :] = features[k][:, 128:256]
    t_s[...] = jnp.zeros(t_s.shape, F32)
    row_b = row_i.astype(F32).astype(BF16)
    for c in range(16):
        place = jnp.where(row_b == rank[c : c + 1].astype(BF16), jnp.bfloat16(1.0), jnp.bfloat16(0.0))
        both = jnp.concatenate([feat0[c * STRIDE : c * STRIDE + KD, :], feat1[c * STRIDE : c * STRIDE + KD, :]], 1)
        sorted_s[c, 0:PS, :] = dot(place, both.astype(BF16), ((1,), (1,)))
        sorted_s[c, PS : PS + MOVE, :] = jnp.zeros((MOVE, KD), F32)
    copy.wait()
    for q in range(4):

        def place_of(c, q=q):
            return meta_s[21, q * 16 + c], meta_s[21, 64 + q * 16 + c], meta_s[22, q * 16 + c]

        @pl.when(meta_s[23, q] <= MOVE)
        def _():
            for c in range(16):
                source, _, target = place_of(c)
                t_s[pl.ds(target, MOVE), :] = sorted_s[c, pl.ds(source, MOVE), :]

        @pl.when(meta_s[23, q] > MOVE)
        def _():
            def append(c, carry):
                source, count, target = place_of(c)

                def chunk(i, carry):
                    t_s[pl.ds(target + 64 * i, 64), :] = sorted_s[c, pl.ds(source + 64 * i, 64), :]
                    return carry

                return lax.fori_loop(0, (count + 63) // 64, chunk, carry)

            lax.fori_loop(0, 16, append, 0)

    t_out[...] = t_s[...].astype(BF16)


def pair_kernel(pencils, fields, group, n_in, role, *refs):
    table, shift = refs[0], refs[1]
    inputs = refs[2 : 2 + n_in]
    targets = refs[2 + n_in]
    refs = refs[3 + n_in :]
    if role == "last":
        rank_ref, _, _, out, acc1, acc2, back = refs[:7]
        refs = refs[7:]
    elif role == "next":
        acc1, acc2 = refs[2:4]
        refs = refs[4:]
    else:
        acc1, acc2 = refs[:2]
        refs = refs[2:]
        acc1[...] = jnp.zeros(acc1.shape, F32)
        acc2[...] = jnp.zeros(acc2.shape, F32)
    roll_s, stage0, stage1, weights, c_lo, c_hi, squares = refs
    row_i = lax.broadcasted_iota(jnp.int32, (RC, PS), 0).astype(F32)
    for p, (which, index, dy, dz) in enumerate(pencils):
        start = 15 if dy == 0 else lax.rem(shift[0 if dy < 0 else 1] + 15, 16)
        rolled = []
        for f in range(4):
            value = inputs[which][index, f]
            for half in range(2):
                part = value[:, half * 128 : half * 128 + 128]
                for copy in range(3):
                    roll_s[p, 2 * f + half, copy * 16 : copy * 16 + 16, :] = part
            rolled.append(
                jnp.concatenate([roll_s[p, 2 * f, pl.ds(start, RC), :], roll_s[p, 2 * f + 1, pl.ds(start, RC), :]], 1)
            )
        y, x, z, m = rolled
        y = y + float(dy)
        z = z + float(dz)
        x = x + (row_i - 9.0)
        live = (m > 0.0) & (row_i < 18.0)
        cube = jnp.where(live, m, 1.0) * (16.0 / 3.141592653589793)
        c = jnp.where(live, jnp.exp2(jnp.log2(cube) * (1.0 / 3.0)), 0.0)
        w = c * c * 16.0
        norm = w * (y * y + x * x + z * z)
        w2 = w * -2.0
        py, pz, px, pw, pn = pieces(y * w2), pieces(z * w2), pieces(x * w2), pieces(w), pieces(norm)
        features = [py[b] for _, b in SHORT] + [pz[b] for _, b in SHORT] + [px[b] for _, b in FULL] + [pw[b] for _, b in FULL]
        features = features + list(pn) + [jnp.zeros((RC, PS), F32)]
        for k in range(KD):
            stage0[p, pl.ds(k, RC, stride=STRIDE), :] = features[k][:, 0:128]
            stage1[p, pl.ds(k, RC, stride=STRIDE), :] = features[k][:, 128:256]
        c_lo[pl.ds(p * RC, RC), :] = c[:, 0:128]
        c_hi[pl.ds(p * RC, RC), :] = c[:, 128:256]
        for r in range(RC):
            if r < 18 or r == 23:
                weights[p * RC + r, :, 0:128] = stage0[p, r * STRIDE : r * STRIDE + KD, :].astype(BF16)
                weights[p * RC + r, :, 128:256] = stage1[p, r * STRIDE : r * STRIDE + KD, :].astype(BF16)

    def decode(i):
        return pl.multiple_of(table[i], 16), [table[i + ITEMS * field] for field in fields]

    def multiply(i, slot):
        at, sources = decode(i)
        lhs = targets[pl.ds(at, BLOCK), :]
        for n, source in enumerate(sources):
            slot[:, 256 * n : 256 * n + 256] = dot(lhs, weights[source])

    def consume(i, slot):
        at, sources = decode(i)
        cs = [ref[pl.ds(source, 8, stride=0), :] for source in sources for ref in (c_lo, c_hi)]
        for g in range(BLOCK // 8):
            sum1 = acc1[pl.ds(at + 8 * g, 8), :]
            sum2 = acc2[pl.ds(at + 8 * g, 8), :]
            for t, scale in enumerate(cs):
                square = jnp.maximum(slot[8 * g : 8 * g + 8, 128 * t : 128 * t + 128], 1e-30)
                root = square * lax.rsqrt(square)
                inner = scale - root
                outer = jnp.maximum(inner + scale, 0.0)
                inner = jnp.maximum(inner, 0.0)
                sum1 = sum1 + outer * outer * outer
                sum2 = sum2 + inner * inner * inner
            acc1[pl.ds(at + 8 * g, 8), :] = sum1
            acc2[pl.ds(at + 8 * g, 8), :] = sum2

    count = table[META]
    for k in range(group):
        multiply(k, squares.at[k])

    def step(it, carry):
        i = it * group
        for k in range(group):
            consume(i + k, squares.at[k])
        for k in range(group):
            multiply(i + group + k, squares.at[k])
        return carry

    lax.fori_loop(0, (count + group - 1) // group, step, 0)

    if role == "last":
        unsort(table, acc1, acc2, back, rank_ref, out)


def unsort(table, acc1, acc2, back, rank_ref, out):
    for q in range(4):

        def place_of(c, q=q):
            at = META + 128 + q * 16 + c
            return table[at], table[at + 64], table[at + 128]

        @pl.when(table[META + 384 + q] <= MOVE)
        def _():
            for c in range(16):
                target, _, source = place_of(c)
                value = acc1[pl.ds(source, MOVE), :] - 4.0 * acc2[pl.ds(source, MOVE), :]
                back[c, pl.ds(target, MOVE), :] = value

        @pl.when(table[META + 384 + q] > MOVE)
        def _():
            def fetch(c, carry):
                target, length, source = place_of(c)

                def chunk(i, carry):
                    value = acc1[pl.ds(source + 64 * i, 64), :] - 4.0 * acc2[pl.ds(source + 64 * i, 64), :]
                    back[c, pl.ds(target + 64 * i, 64), :] = value
                    return carry

                return lax.fori_loop(0, (length + 63) // 64, chunk, carry)

            lax.fori_loop(0, 16, fetch, 0)

    row_f = lax.broadcasted_iota(jnp.int32, (PS, 128), 0).astype(F32)
    ones = jnp.ones((256, 128), BF16)
    for c in range(16):
        value = back[c, 0:PS, :]
        high = value.astype(BF16)
        low = (value - high.astype(F32)).astype(BF16)
        sums = dot(jnp.concatenate([high, low], 1), ones)
        for half in range(2):
            lanes = slice(128 * half, 128 * half + 128)
            mine = row_f == rank_ref[c : c + 1, lanes]
            out[c : c + 1, lanes] = jnp.sum(jnp.where(mine, sums, 0.0), 0, keepdims=True)


VMEM_SPEC = pl.BlockSpec(memory_space=pltpu.VMEM)
SMEM_SPEC = pl.BlockSpec(memory_space=pltpu.SMEM)


def prepare(data, interpret=False):
    return pl.pallas_call(
        prep_kernel,
        out_shape=(
            jax.ShapeDtypeStruct((ROWS, KD), BF16),
            jax.ShapeDtypeStruct((NX, PS), F32),
            jax.ShapeDtypeStruct((24, 128), jnp.int32),
        ),
        in_specs=[VMEM_SPEC],
        out_specs=[VMEM_SPEC] * 3,
        scratch_shapes=[
            pltpu.VMEM((16 * STRIDE, 128), F32),
            pltpu.VMEM((16 * STRIDE, 128), F32),
            pltpu.VMEM((16, PS + MOVE, KD), F32),
            pltpu.VMEM((ROWS, KD), F32),
            pltpu.VMEM((24, 128), jnp.int32),
            pltpu.SMEM((24, 128), jnp.int32),
            pltpu.SemaphoreType.DMA,
        ],
        compiler_params=pltpu.CompilerParams(vmem_limit_bytes=40 << 20),
        interpret=interpret,
        name="prepare",
    )(data)


def pair_sums(pencils, fields, group, role, table, shift, inputs, targets, rest, name, interpret=False):
    n = len(pencils)
    out_shape = [jax.ShapeDtypeStruct((ROWS, 128), F32)] * 2
    first_in, first_out = len(inputs) + 3, 0
    scratch = [
        pltpu.VMEM((n, 8, 48, 128), F32),
        pltpu.VMEM((n, RC * STRIDE, 128), F32),
        pltpu.VMEM((n, RC * STRIDE, 128), F32),
        pltpu.VMEM((n * RC, KD, PS), BF16),
        pltpu.VMEM((n * RC, 128), F32),
        pltpu.VMEM((n * RC, 128), F32),
        pltpu.VMEM((group, BLOCK, PS * len(fields)), F32),
    ]
    if role == "last":
        out_shape = [jax.ShapeDtypeStruct((NX, PS), F32)] + out_shape
        first_in, first_out = first_in + 1, 1
        scratch = [pltpu.VMEM((NX, PS + MOVE, 128), F32)] + scratch
    aliases = {} if role == "first" else {first_in: first_out, first_in + 1: first_out + 1}
    return pl.pallas_call(
        functools.partial(pair_kernel, pencils, fields, group, len(inputs), role),
        out_shape=out_shape,
        in_specs=[SMEM_SPEC] * 2 + [VMEM_SPEC] * (len(inputs) + 1 + len(rest)),
        out_specs=[VMEM_SPEC] * len(out_shape),
        scratch_shapes=scratch,
        input_output_aliases=aliases,
        compiler_params=pltpu.CompilerParams(vmem_limit_bytes=40 << 20),
        interpret=interpret,
        name=name,
    )(table, shift, *inputs, targets, *rest)


OWN = ((0, 0, 0, 0),)
SIDE = ((0, 0, -1, 0), (1, 0, 1, 0))
FAR = ((0, 0, 0, -1), (1, 0, 0, 1), (0, 1, -1, -1), (1, 1, -1, 1), (0, 2, 1, -1), (1, 2, 1, 1))


def own_sums(table, shift, data, targets):
    return pair_sums(OWN, (1,), 16, "first", table, shift, [data[None]], targets, [], "own")


def side_sums(table, shift, below, above, targets, sums):
    return pair_sums(SIDE, (2,), 16, "next", table, shift, [below[None], above[None]], targets, sums, "side")


def far_sums(table, shift, low, high, targets, rank, sums):
    return pair_sums(FAR, (3, 4), 8, "last", table, shift, [low, high], targets, [rank, *sums], "far")[0]


def ring(axis, distance):
    count = lax.axis_size(axis)
    return [(i, (i + distance) % count) for i in range(count)]


def shards(positions, masses, counts, shear_offset):
    slot_index = lax.broadcasted_iota(jnp.int32, masses.shape, 3)
    weight = jnp.where(slot_index < counts[..., None], masses, jnp.float32(0.0))
    data = jnp.concatenate([positions, weight[None]], 0).reshape(4, NX, PS)
    index = lax.axis_index("shear")
    offset = shear_offset[0]
    shift = jnp.stack([
        jnp.where(index == 0, NX - offset, 0),
        jnp.where(index == lax.axis_size("shear") - 1, offset, 0),
    ]).astype(jnp.int32)
    below = lax.ppermute(data, "shear", ring("shear", 1))
    above = lax.ppermute(data, "shear", ring("shear", -1))
    targets, rank, table = prepare(data)
    table = table.reshape(-1)
    sums = own_sums(table, shift, data, targets)
    rows = jnp.stack([data, below, above])
    rows, targets, rank, table, shift, sums = lax.optimization_barrier((rows, targets, rank, table, shift, sums))
    low = lax.ppermute(rows, "cross", ring("cross", 1))
    high = lax.ppermute(rows, "cross", ring("cross", -1))
    sums = side_sums(table, shift, rows[1], rows[2], targets, sums)
    density = far_sums(table, shift, low, high, targets, rank, sums)
    return density.reshape(masses.shape)


def solution(mesh):
    in_specs = (
        P(None, "shear", None, "cross", None),
        P("shear", None, "cross", None),
        P("shear", None, "cross"),
        P(),
    )
    out_specs = P("shear", None, "cross", None)
    return jax.shard_map(shards, mesh=mesh, in_specs=in_specs, out_specs=out_specs, check_vma=False)
```

```python
import functools

import jax
import jax.numpy as jnp
from jax import lax
from jax.experimental import pallas as pl
from jax.experimental.pallas import tpu as pltpu
from jax.sharding import PartitionSpec as P

NX = 16
PS = 256
ROWS = 4480
NULL_ROW = 4416
BLOCK = 32
GAP = 48
MOVE = 96
RC = 24
STRIDE = 33
KD = 32
ITEMS = 512
META = 5 * ITEMS
F32 = jnp.float32
BF16 = jnp.bfloat16

FULL = [(0, 0), (0, 1), (0, 2), (1, 0), (1, 1), (1, 2), (2, 0), (2, 1)]
SHORT = [(0, 0), (0, 1), (0, 2), (1, 0), (1, 1), (2, 0)]


def pieces(value):
    first = value.astype(BF16).astype(F32)
    rest = value - first
    second = rest.astype(BF16).astype(F32)
    return first, second, rest - second


def dot(a, b, dims=((1,), (0,))):
    return lax.dot_general(a, b, (dims, ((), ())), preferred_element_type=F32)


def steps(value, width, most):
    return sum((value >= width * (i + 1)).astype(jnp.int32) for i in range(most))


def prep_kernel(data, t_out, rank_out, list_out, feat0, feat1, sorted_s, t_s, meta_v, meta_s, sem):
    y, x, z, m = data[0], data[1], data[2], data[3]
    valid = m > 0.0
    one = jnp.float32(1.0)
    nil = jnp.float32(0.0)
    code = jnp.where(y >= 0.5, 4.0, 0.0) + jnp.where(z >= 0.5, 2.0, 0.0) + jnp.where(x >= 0.5, 1.0, 0.0)
    code = jnp.where(valid, code, 9.0)
    masks = [jnp.where(code == float(b), one, nil) for b in range(8)]
    stacked = jnp.concatenate(masks, 0).astype(BF16)
    row_i = lax.broadcasted_iota(jnp.int32, (PS, PS), 0)
    lane_i = lax.broadcasted_iota(jnp.int32, (PS, PS), 1)
    upper = jnp.where(row_i <= lane_i, one, nil).astype(BF16)
    running = dot(stacked, upper)
    total = dot(stacked, jnp.ones((PS, 128), BF16))
    begin = jnp.zeros((16, 128), F32)
    rank = jnp.zeros((16, PS), F32)
    for b in range(8):
        wide = jnp.concatenate([begin, begin], 1)
        rank = rank + masks[b] * (wide + running[b * 16 : b * 16 + 16] - 1.0)
        begin = begin + total[b * 16 : b * 16 + 16]
    rank = jnp.where(valid, rank, -1.0)
    rank_out[...] = rank

    g = lax.broadcasted_iota(jnp.int32, (200, 128), 0)
    j = lax.broadcasted_iota(jnp.int32, (200, 128), 1)
    kind = steps(g, 96, 2)
    g = g - 96 * kind
    group_q = steps(g, RC, 3)
    group_x = g - RC * group_q - 1
    limit = jnp.where(kind == 0, 2 * group_x - 1, jnp.where(group_x > 16, 0, 2 * group_x + 3))
    limit = jnp.where((kind == 0) & (group_x > 16), 0, limit)
    limit = jnp.where(kind == 2, 32, limit)
    group_q = jnp.where(kind == 2, g, group_q)
    spot = 2 * (j & 15) + ((j >> 4) & 1)
    counted = ((j >> 5) == group_q) & (spot < limit)
    columns = dot(jnp.where(counted, one, nil).astype(BF16), total.astype(BF16))
    base = [jnp.zeros((1, 128), F32)]
    for q in range(3):
        end = base[q] + columns[192 + q : 193 + q] + float(GAP + 15)
        base.append(jnp.floor(end * 0.0625) * 16.0)
    base_col = jnp.concatenate([jnp.broadcast_to(b, (RC, 128)) for b in base], 0)
    low, high = columns[0:96], columns[96:192]
    first = jnp.floor((low + base_col) * 0.0625) * 16.0
    n_blocks = jnp.floor((high + base_col - first + float(BLOCK - 1)) * (1.0 / BLOCK))
    n_blocks = jnp.where(high > low, n_blocks, 0.0)
    gi = lax.broadcasted_iota(jnp.int32, (96, 96), 0)
    gj = lax.broadcasted_iota(jnp.int32, (96, 96), 1)
    before = dot(jnp.where(gj < gi, one, nil).astype(BF16), n_blocks.astype(BF16))
    group_r = lax.broadcasted_iota(jnp.int32, (96, 128), 0)
    group_q = steps(group_r, RC, 3)
    cell_r = group_r - group_q * RC
    fields = [
        cell_r,
        cell_r + RC * (group_q >> 1),
        cell_r + RC * (group_q & 1),
        cell_r + RC * (2 + group_q),
    ]
    lane96 = lax.broadcasted_iota(jnp.int32, (96, 128), 1).astype(F32)
    away = [lane96 + float(128 * t) - before for t in range(4)]
    inside = [(v >= 0.0) & (v < n_blocks) for v in away]
    out_rows = []
    for t in range(4):
        entry = first + away[t] * float(BLOCK) - float(NULL_ROW)
        out_rows.append(jnp.sum(jnp.where(inside[t], entry, 0.0), 0, keepdims=True) + float(NULL_ROW))
    for field in fields:
        entry = field.astype(F32) - float(RC - 1)
        for t in range(4):
            out_rows.append(jnp.sum(jnp.where(inside[t], entry, 0.0), 0, keepdims=True) + float(RC - 1))
    out_rows.append(before[95:96] + n_blocks[95:96])
    total_row = dot(jnp.ones((8, PS), BF16), stacked, ((1,), (1,)))
    j = lax.broadcasted_iota(jnp.int32, (128, 256), 0)
    k = lax.broadcasted_iota(jnp.int32, (128, 256), 1)
    quad, kind, goal = j >> 5, k >> 6, (k & 63) >> 4
    same, earlier = (j & 15) == (k & 15), (j & 15) < (k & 15)
    counted = ((kind == 0) & same & (quad < goal)) | ((kind == 1) & same & (quad == goal))
    counted = counted | ((kind == 2) & earlier & (quad == goal))
    meta = dot(total_row.astype(BF16), jnp.where(counted, one, nil).astype(BF16))
    lane1 = lax.broadcasted_iota(jnp.int32, (1, 128), 1)
    base_lane = jnp.where(lane1 < 16, base[0], jnp.where(lane1 < 32, base[1], jnp.where(lane1 < 48, base[2], base[3])))
    out_rows.append(meta[0:1, 0:128])
    out_rows.append(meta[0:1, 128:256] + base_lane)
    longest = jnp.where(lane1 >= 64, meta[0:1, 0:128], 0.0)
    flags = jnp.zeros((1, 128), F32)
    for q in range(4):
        top = jnp.max(jnp.where((lane1 >= 64 + 16 * q) & (lane1 < 80 + 16 * q), longest, 0.0), 1, keepdims=True)
        flags = jnp.where(lane1 == q, top, flags)
    out_rows.append(flags)
    table = jnp.concatenate(out_rows, 0).astype(jnp.int32)
    list_out[...] = table
    meta_v[...] = table
    copy = pltpu.make_async_copy(meta_v, meta_s, sem)
    copy.start()

    cell_i = lax.broadcasted_iota(jnp.int32, (16, PS), 0).astype(F32)
    xg = x + (cell_i - 8.0)
    norm = y * y + xg * xg + z * z
    py, pz, px, pn = pieces(y), pieces(z), pieces(xg), pieces(norm)
    features = [py[a] for a, _ in SHORT] + [pz[a] for a, _ in SHORT] + [px[a] for a, _ in FULL] + [pn[a] for a, _ in FULL]
    ones = jnp.ones((16, PS), F32)
    features = features + [ones, ones, ones, jnp.zeros((16, PS), F32)]
    for k in range(KD):
        feat0[pl.ds(k, 16, stride=STRIDE), :] = features[k][:, 0:128]
        feat1[pl.ds(k, 16, stride=STRIDE), :] = features[k][:, 128:256]
    t_s[...] = jnp.zeros(t_s.shape, F32)
    row_b = row_i.astype(F32).astype(BF16)
    for c in range(16):
        place = jnp.where(row_b == rank[c : c + 1].astype(BF16), jnp.bfloat16(1.0), jnp.bfloat16(0.0))
        both = jnp.concatenate([feat0[c * STRIDE : c * STRIDE + KD, :], feat1[c * STRIDE : c * STRIDE + KD, :]], 1)
        sorted_s[c, 0:PS, :] = dot(place, both.astype(BF16), ((1,), (1,)))
        sorted_s[c, PS : PS + MOVE, :] = jnp.zeros((MOVE, KD), F32)
    copy.wait()
    for q in range(4):

        def place_of(c, q=q):
            return meta_s[21, q * 16 + c], meta_s[21, 64 + q * 16 + c], meta_s[22, q * 16 + c]

        @pl.when(meta_s[23, q] <= MOVE)
        def _():
            for c in range(16):
                source, _, target = place_of(c)
                t_s[pl.ds(target, MOVE), :] = sorted_s[c, pl.ds(source, MOVE), :]

        @pl.when(meta_s[23, q] > MOVE)
        def _():
            def append(c, carry):
                source, count, target = place_of(c)

                def chunk(i, carry):
                    t_s[pl.ds(target + 64 * i, 64), :] = sorted_s[c, pl.ds(source + 64 * i, 64), :]
                    return carry

                return lax.fori_loop(0, (count + 63) // 64, chunk, carry)

            lax.fori_loop(0, 16, append, 0)

    t_out[...] = t_s[...].astype(BF16)


def pair_kernel(pencils, fields, group, n_in, role, *refs):
    inputs = refs[2 : 2 + n_in]
    table, shift, table_sem, shift_sem = refs[-4:]
    table_copy = pltpu.make_async_copy(refs[0], table, table_sem)
    shift_copy = pltpu.make_async_copy(refs[1], shift, shift_sem)
    shift_copy.start()
    table_copy.start()
    shift_here = False
    refs = refs[:-4]
    targets = refs[2 + n_in]
    refs = refs[3 + n_in :]
    if role == "last":
        rank_ref, _, _, out, acc1, acc2, back, rows_out, out_sem = refs[:9]
        refs = refs[9:]
    elif role == "next":
        acc1, acc2 = refs[2:4]
        refs = refs[4:]
    else:
        acc1, acc2 = refs[:2]
        refs = refs[2:]
        acc1[...] = jnp.zeros(acc1.shape, F32)
        acc2[...] = jnp.zeros(acc2.shape, F32)
    roll_s, stage0, stage1, weights, c_lo, c_hi, squares = refs
    row_i = lax.broadcasted_iota(jnp.int32, (RC, PS), 0).astype(F32)
    for p, (which, index, dy, dz) in enumerate(pencils):
        if dy != 0 and not shift_here:
            shift_copy.wait()
            shift_here = True
        start = 15 if dy == 0 else lax.rem(shift[0 if dy < 0 else 1] + 15, 16)
        rolled = []
        for f in range(4):
            value = inputs[which][index, f]
            for half in range(2):
                part = value[:, half * 128 : half * 128 + 128]
                for copy in range(3):
                    roll_s[p, 2 * f + half, copy * 16 : copy * 16 + 16, :] = part
            rolled.append(
                jnp.concatenate([roll_s[p, 2 * f, pl.ds(start, RC), :], roll_s[p, 2 * f + 1, pl.ds(start, RC), :]], 1)
            )
        y, x, z, m = rolled
        y = y + float(dy)
        z = z + float(dz)
        x = x + (row_i - 9.0)
        live = (m > 0.0) & (row_i < 18.0)
        cube = jnp.where(live, m, 1.0) * (16.0 / 3.141592653589793)
        c = jnp.where(live, jnp.exp2(jnp.log2(cube) * (1.0 / 3.0)), 0.0)
        w = c * c * 16.0
        norm = w * (y * y + x * x + z * z)
        w2 = w * -2.0
        py, pz, px, pw, pn = pieces(y * w2), pieces(z * w2), pieces(x * w2), pieces(w), pieces(norm)
        features = [py[b] for _, b in SHORT] + [pz[b] for _, b in SHORT] + [px[b] for _, b in FULL] + [pw[b] for _, b in FULL]
        features = features + list(pn) + [jnp.zeros((RC, PS), F32)]
        for k in range(KD):
            stage0[p, pl.ds(k, RC, stride=STRIDE), :] = features[k][:, 0:128]
            stage1[p, pl.ds(k, RC, stride=STRIDE), :] = features[k][:, 128:256]
        c_lo[pl.ds(p * RC, RC), :] = c[:, 0:128]
        c_hi[pl.ds(p * RC, RC), :] = c[:, 128:256]
        for r in range(RC):
            if r < 18 or r == 23:
                weights[p * RC + r, :, 0:128] = stage0[p, r * STRIDE : r * STRIDE + KD, :].astype(BF16)
                weights[p * RC + r, :, 128:256] = stage1[p, r * STRIDE : r * STRIDE + KD, :].astype(BF16)

    def decode(i):
        return pl.multiple_of(table[i], 16), [table[i + ITEMS * field] for field in fields]

    def multiply(i, slot):
        at, sources = decode(i)
        lhs = targets[pl.ds(at, BLOCK), :]
        for n, source in enumerate(sources):
            slot[:, 256 * n : 256 * n + 256] = dot(lhs, weights[source])

    def consume(i, slot):
        at, sources = decode(i)
        cs = [ref[pl.ds(source, 8, stride=0), :] for source in sources for ref in (c_lo, c_hi)]
        for g in range(BLOCK // 8):
            sum1 = acc1[pl.ds(at + 8 * g, 8), :]
            sum2 = acc2[pl.ds(at + 8 * g, 8), :]
            for t, scale in enumerate(cs):
                square = jnp.maximum(slot[8 * g : 8 * g + 8, 128 * t : 128 * t + 128], 1e-30)
                root = square * lax.rsqrt(square)
                inner = scale - root
                outer = jnp.maximum(inner + scale, 0.0)
                inner = jnp.maximum(inner, 0.0)
                sum1 = sum1 + outer * outer * outer
                sum2 = sum2 + inner * inner * inner
            acc1[pl.ds(at + 8 * g, 8), :] = sum1
            acc2[pl.ds(at + 8 * g, 8), :] = sum2

    if not shift_here:
        shift_copy.wait()
    table_copy.wait()
    count = table[META]
    for k in range(group):
        multiply(k, squares.at[k])

    def step(it, carry):
        i = it * group
        for k in range(group):
            consume(i + k, squares.at[k])
        for k in range(group):
            multiply(i + group + k, squares.at[k])
        return carry

    lax.fori_loop(0, (count + group - 1) // group, step, 0)

    if role == "last":
        unsort(table, acc1, acc2, back, rank_ref, rows_out, out, out_sem)


def unsort(table, acc1, acc2, back, rank_ref, rows_out, out, out_sem):
    for q in range(4):

        def place_of(c, q=q):
            at = META + 128 + q * 16 + c
            return table[at], table[at + 64], table[at + 128]

        @pl.when(table[META + 384 + q] <= MOVE)
        def _():
            for c in range(16):
                target, _, source = place_of(c)
                value = acc1[pl.ds(source, MOVE), :] - 4.0 * acc2[pl.ds(source, MOVE), :]
                back[c, pl.ds(target, MOVE), :] = value

        @pl.when(table[META + 384 + q] > MOVE)
        def _():
            def fetch(c, carry):
                target, length, source = place_of(c)

                def chunk(i, carry):
                    value = acc1[pl.ds(source + 64 * i, 64), :] - 4.0 * acc2[pl.ds(source + 64 * i, 64), :]
                    back[c, pl.ds(target + 64 * i, 64), :] = value
                    return carry

                return lax.fori_loop(0, (length + 63) // 64, chunk, carry)

            lax.fori_loop(0, 16, fetch, 0)

    row_f = lax.broadcasted_iota(jnp.int32, (PS, 128), 0).astype(F32)
    ones = jnp.ones((256, 128), BF16)
    for c in range(16):
        value = back[c, 0:PS, :]
        high = value.astype(BF16)
        low = (value - high.astype(F32)).astype(BF16)
        sums = dot(jnp.concatenate([high, low], 1), ones)
        for half in range(2):
            lanes = slice(128 * half, 128 * half + 128)
            mine = row_f == rank_ref[c : c + 1, lanes]
            rows_out[0, c, :, lanes] = jnp.sum(jnp.where(mine, sums, 0.0), 0, keepdims=True)
    copy = pltpu.make_async_copy(rows_out, out, out_sem)
    copy.start()
    copy.wait()


VMEM_SPEC = pl.BlockSpec(memory_space=pltpu.VMEM)
HBM_SPEC = pl.BlockSpec(memory_space=pl.ANY)


def prepare(data, interpret=False):
    return pl.pallas_call(
        prep_kernel,
        out_shape=(
            jax.ShapeDtypeStruct((ROWS, KD), BF16),
            jax.ShapeDtypeStruct((NX, PS), F32),
            jax.ShapeDtypeStruct((24, 128), jnp.int32),
        ),
        in_specs=[VMEM_SPEC],
        out_specs=[VMEM_SPEC] * 3,
        scratch_shapes=[
            pltpu.VMEM((16 * STRIDE, 128), F32),
            pltpu.VMEM((16 * STRIDE, 128), F32),
            pltpu.VMEM((16, PS + MOVE, KD), F32),
            pltpu.VMEM((ROWS, KD), F32),
            pltpu.VMEM((24, 128), jnp.int32),
            pltpu.SMEM((24, 128), jnp.int32),
            pltpu.SemaphoreType.DMA,
        ],
        compiler_params=pltpu.CompilerParams(vmem_limit_bytes=40 << 20),
        interpret=interpret,
        name="prepare",
    )(data)


def pair_sums(pencils, fields, group, role, table, shift, inputs, targets, rest, name, interpret=False):
    n = len(pencils)
    out_shape = [jax.ShapeDtypeStruct((ROWS, 128), F32)] * 2
    out_specs = [VMEM_SPEC] * 2
    first_in, first_out = len(inputs) + 3, 0
    scratch = [
        pltpu.VMEM((n, 8, 48, 128), F32),
        pltpu.VMEM((n, RC * STRIDE, 128), F32),
        pltpu.VMEM((n, RC * STRIDE, 128), F32),
        pltpu.VMEM((n * RC, KD, PS), BF16),
        pltpu.VMEM((n * RC, 128), F32),
        pltpu.VMEM((n * RC, 128), F32),
        pltpu.VMEM((group, BLOCK, PS * len(fields)), F32),
    ]
    if role == "last":
        out_shape = [jax.ShapeDtypeStruct((1, NX, 1, PS), F32)] + out_shape
        first_in, first_out = first_in + 1, 1
        out_specs = [HBM_SPEC] + out_specs
        scratch = [pltpu.VMEM((NX, PS + MOVE, 128), F32), pltpu.VMEM((1, NX, 1, PS), F32), pltpu.SemaphoreType.DMA] + scratch
    scratch = scratch + [
        pltpu.SMEM((24 * 128,), jnp.int32),
        pltpu.SMEM((2,), jnp.int32),
        pltpu.SemaphoreType.DMA,
        pltpu.SemaphoreType.DMA,
    ]
    aliases = {} if role == "first" else {first_in: first_out, first_in + 1: first_out + 1}
    return pl.pallas_call(
        functools.partial(pair_kernel, pencils, fields, group, len(inputs), role),
        out_shape=out_shape,
        in_specs=[VMEM_SPEC] * (len(inputs) + 3 + len(rest)),
        out_specs=out_specs,
        scratch_shapes=scratch,
        input_output_aliases=aliases,
        compiler_params=pltpu.CompilerParams(vmem_limit_bytes=40 << 20),
        interpret=interpret,
        name=name,
    )(table, shift, *inputs, targets, *rest)


OWN = ((0, 0, 0, 0),)
SIDE = ((0, 0, -1, 0), (1, 0, 1, 0))
FAR = ((0, 0, 0, -1), (1, 0, 0, 1), (0, 1, -1, -1), (1, 1, -1, 1), (0, 2, 1, -1), (1, 2, 1, 1))


def own_sums(table, shift, data, targets):
    return pair_sums(OWN, (1,), 16, "first", table, shift, [data[None]], targets, [], "own")


def side_sums(table, shift, below, above, targets, sums):
    return pair_sums(SIDE, (2,), 16, "next", table, shift, [below[None], above[None]], targets, sums, "side")


def far_sums(table, shift, low, high, targets, rank, sums):
    return pair_sums(FAR, (3, 4), 8, "last", table, shift, [low, high], targets, [rank, *sums], "far")[0]


def ring(axis, distance):
    count = lax.axis_size(axis)
    return [(i, (i + distance) % count) for i in range(count)]


def shards(positions, masses, counts, shear_offset):
    slot_index = lax.broadcasted_iota(jnp.int32, masses.shape, 3)
    weight = jnp.where(slot_index < counts[..., None], masses, jnp.float32(0.0))
    data = jnp.concatenate([positions, weight[None]], 0).reshape(4, NX, PS)
    index = lax.axis_index("shear")
    offset = shear_offset[0]
    shift = jnp.stack([
        jnp.where(index == 0, NX - offset, 0),
        jnp.where(index == lax.axis_size("shear") - 1, offset, 0),
    ]).astype(jnp.int32)
    below = lax.ppermute(data, "shear", ring("shear", 1))
    above = lax.ppermute(data, "shear", ring("shear", -1))
    targets, rank, table = prepare(data)
    table = table.reshape(-1)
    sums = own_sums(table, shift, data, targets)
    rows = jnp.stack([data, below, above])
    rows, targets, rank, table, shift, sums = lax.optimization_barrier((rows, targets, rank, table, shift, sums))
    low = lax.ppermute(rows, "cross", ring("cross", 1))
    high = lax.ppermute(rows, "cross", ring("cross", -1))
    sums = side_sums(table, shift, rows[1], rows[2], targets, sums)
    density = far_sums(table, shift, low, high, targets, rank, sums)
    return density


def solution(mesh):
    in_specs = (
        P(None, "shear", None, "cross", None),
        P("shear", None, "cross", None),
        P("shear", None, "cross"),
        P(),
    )
    out_specs = P("shear", None, "cross", None)
    return jax.shard_map(shards, mesh=mesh, in_specs=in_specs, out_specs=out_specs, check_vma=False)
```

```python
import functools

import jax
import jax.numpy as jnp
from jax import lax
from jax.experimental import pallas as pl
from jax.experimental.pallas import tpu as pltpu
from jax.sharding import PartitionSpec as P


NX = 16
PS = 256
ROWS = 4480
NULL_ROW = 4416
BLOCK = 32
GAP = 48
MOVE = 96
RC = 24
STRIDE = 33
KD = 32
ITEMS = 512
META = 5 * ITEMS
F32 = jnp.float32
BF16 = jnp.bfloat16

FULL = [(0, 0), (0, 1), (0, 2), (1, 0), (1, 1), (1, 2), (2, 0), (2, 1)]
SHORT = [(0, 0), (0, 1), (0, 2), (1, 0), (1, 1), (2, 0)]


def pieces(value):
    first = value.astype(BF16).astype(F32)
    rest = value - first
    second = rest.astype(BF16).astype(F32)
    return first, second, rest - second


def dot(a, b, dims=((1,), (0,))):
    return lax.dot_general(a, b, (dims, ((), ())), preferred_element_type=F32)


def steps(value, width, most):
    return sum((value >= width * (i + 1)).astype(jnp.int32) for i in range(most))


def prep_kernel(data, t_out, rank_out, list_out, feat0, feat1, sorted_s, t_s, meta_v, meta_s, sem):
    y, x, z, m = data[0], data[1], data[2], data[3]
    valid = m > 0.0
    one = jnp.float32(1.0)
    nil = jnp.float32(0.0)
    code = jnp.where(y >= 0.5, 4.0, 0.0) + jnp.where(z >= 0.5, 2.0, 0.0) + jnp.where(x >= 0.5, 1.0, 0.0)
    code = jnp.where(valid, code, 9.0)
    masks = [jnp.where(code == float(b), one, nil) for b in range(8)]
    stacked = jnp.concatenate(masks, 0).astype(BF16)
    row_i = lax.broadcasted_iota(jnp.int32, (PS, PS), 0)
    lane_i = lax.broadcasted_iota(jnp.int32, (PS, PS), 1)
    upper = jnp.where(row_i <= lane_i, one, nil).astype(BF16)
    running = dot(stacked, upper)
    total = dot(stacked, jnp.ones((PS, 128), BF16))
    begin = jnp.zeros((16, 128), F32)
    rank = jnp.zeros((16, PS), F32)
    for b in range(8):
        wide = jnp.concatenate([begin, begin], 1)
        rank = rank + masks[b] * (wide + running[b * 16 : b * 16 + 16] - 1.0)
        begin = begin + total[b * 16 : b * 16 + 16]
    rank = jnp.where(valid, rank, -1.0)
    rank_out[...] = rank

    g = lax.broadcasted_iota(jnp.int32, (200, 128), 0)
    j = lax.broadcasted_iota(jnp.int32, (200, 128), 1)
    kind = steps(g, 96, 2)
    g = g - 96 * kind
    group_q = steps(g, RC, 3)
    group_x = g - RC * group_q - 1
    limit = jnp.where(kind == 0, 2 * group_x - 1, jnp.where(group_x > 16, 0, 2 * group_x + 3))
    limit = jnp.where((kind == 0) & (group_x > 16), 0, limit)
    limit = jnp.where(kind == 2, 32, limit)
    group_q = jnp.where(kind == 2, g, group_q)
    spot = 2 * (j & 15) + ((j >> 4) & 1)
    counted = ((j >> 5) == group_q) & (spot < limit)
    columns = dot(jnp.where(counted, one, nil).astype(BF16), total.astype(BF16))
    base = [jnp.zeros((1, 128), F32)]
    for q in range(3):
        end = base[q] + columns[192 + q : 193 + q] + float(GAP + 15)
        base.append(jnp.floor(end * 0.0625) * 16.0)
    base_col = jnp.concatenate([jnp.broadcast_to(b, (RC, 128)) for b in base], 0)
    low, high = columns[0:96], columns[96:192]
    first = jnp.floor((low + base_col) * 0.0625) * 16.0
    n_blocks = jnp.floor((high + base_col - first + float(BLOCK - 1)) * (1.0 / BLOCK))
    n_blocks = jnp.where(high > low, n_blocks, 0.0)
    gi = lax.broadcasted_iota(jnp.int32, (96, 96), 0)
    gj = lax.broadcasted_iota(jnp.int32, (96, 96), 1)
    before = dot(jnp.where(gj < gi, one, nil).astype(BF16), n_blocks.astype(BF16))
    group_r = lax.broadcasted_iota(jnp.int32, (96, 128), 0)
    group_q = steps(group_r, RC, 3)
    cell_r = group_r - group_q * RC
    fields = [
        cell_r,
        cell_r + RC * (group_q >> 1),
        cell_r + RC * (group_q & 1),
        cell_r + RC * (2 + group_q),
    ]
    lane96 = lax.broadcasted_iota(jnp.int32, (96, 128), 1).astype(F32)
    away = [lane96 + float(128 * t) - before for t in range(4)]
    inside = [(v >= 0.0) & (v < n_blocks) for v in away]
    out_rows = []
    for t in range(4):
        entry = first + away[t] * float(BLOCK) - float(NULL_ROW)
        out_rows.append(jnp.sum(jnp.where(inside[t], entry, 0.0), 0, keepdims=True) + float(NULL_ROW))
    for field in fields:
        entry = field.astype(F32) - float(RC - 1)
        for t in range(4):
            out_rows.append(jnp.sum(jnp.where(inside[t], entry, 0.0), 0, keepdims=True) + float(RC - 1))
    out_rows.append(before[95:96] + n_blocks[95:96])
    total_row = dot(jnp.ones((8, PS), BF16), stacked, ((1,), (1,)))
    j = lax.broadcasted_iota(jnp.int32, (128, 256), 0)
    k = lax.broadcasted_iota(jnp.int32, (128, 256), 1)
    quad, kind, goal = j >> 5, k >> 6, (k & 63) >> 4
    same, earlier = (j & 15) == (k & 15), (j & 15) < (k & 15)
    counted = ((kind == 0) & same & (quad < goal)) | ((kind == 1) & same & (quad == goal))
    counted = counted | ((kind == 2) & earlier & (quad == goal))
    meta = dot(total_row.astype(BF16), jnp.where(counted, one, nil).astype(BF16))
    lane1 = lax.broadcasted_iota(jnp.int32, (1, 128), 1)
    base_lane = jnp.where(lane1 < 16, base[0], jnp.where(lane1 < 32, base[1], jnp.where(lane1 < 48, base[2], base[3])))
    out_rows.append(meta[0:1, 0:128])
    out_rows.append(meta[0:1, 128:256] + base_lane)
    longest = jnp.where(lane1 >= 64, meta[0:1, 0:128], 0.0)
    flags = jnp.zeros((1, 128), F32)
    for q in range(4):
        top = jnp.max(jnp.where((lane1 >= 64 + 16 * q) & (lane1 < 80 + 16 * q), longest, 0.0), 1, keepdims=True)
        flags = jnp.where(lane1 == q, top, flags)
    out_rows.append(flags)
    table = jnp.concatenate(out_rows, 0).astype(jnp.int32)
    list_out[...] = table
    meta_v[...] = table
    copy = pltpu.make_async_copy(meta_v, meta_s, sem)
    copy.start()

    cell_i = lax.broadcasted_iota(jnp.int32, (16, PS), 0).astype(F32)
    xg = x + (cell_i - 8.0)
    norm = y * y + xg * xg + z * z
    py, pz, px, pn = pieces(y), pieces(z), pieces(xg), pieces(norm)
    features = [py[a] for a, _ in SHORT] + [pz[a] for a, _ in SHORT] + [px[a] for a, _ in FULL] + [pn[a] for a, _ in FULL]
    ones = jnp.ones((16, PS), F32)
    features = features + [ones, ones, ones, jnp.zeros((16, PS), F32)]
    for k in range(KD):
        feat0[pl.ds(k, 16, stride=STRIDE), :] = features[k][:, 0:128]
        feat1[pl.ds(k, 16, stride=STRIDE), :] = features[k][:, 128:256]
    t_s[...] = jnp.zeros(t_s.shape, F32)
    row_b = row_i.astype(F32).astype(BF16)
    for c in range(16):
        place = jnp.where(row_b == rank[c : c + 1].astype(BF16), jnp.bfloat16(1.0), jnp.bfloat16(0.0))
        both = jnp.concatenate([feat0[c * STRIDE : c * STRIDE + KD, :], feat1[c * STRIDE : c * STRIDE + KD, :]], 1)
        sorted_s[c, 0:PS, :] = dot(place, both.astype(BF16), ((1,), (1,)))
        sorted_s[c, PS : PS + MOVE, :] = jnp.zeros((MOVE, KD), F32)
    copy.wait()
    for q in range(4):

        def place_of(c, q=q):
            return meta_s[21, q * 16 + c], meta_s[21, 64 + q * 16 + c], meta_s[22, q * 16 + c]

        @pl.when(meta_s[23, q] <= MOVE)
        def _():
            for c in range(16):
                source, _, target = place_of(c)
                t_s[pl.ds(target, MOVE), :] = sorted_s[c, pl.ds(source, MOVE), :]

        @pl.when(meta_s[23, q] > MOVE)
        def _():
            def append(c, carry):
                source, count, target = place_of(c)

                def chunk(i, carry):
                    t_s[pl.ds(target + 64 * i, 64), :] = sorted_s[c, pl.ds(source + 64 * i, 64), :]
                    return carry

                return lax.fori_loop(0, (count + 63) // 64, chunk, carry)

            lax.fori_loop(0, 16, append, 0)

    t_out[...] = t_s[...].astype(BF16)


def pair_kernel(pencils, fields, group, n_in, role, *refs):
    inputs = refs[2 : 2 + n_in]
    table, shift, table_sem, shift_sem = refs[-4:]
    table_copy = pltpu.make_async_copy(refs[0], table, table_sem)
    shift_copy = pltpu.make_async_copy(refs[1], shift, shift_sem)
    shift_copy.start()
    table_copy.start()
    shift_here = False
    refs = refs[:-4]
    targets = refs[2 + n_in]
    refs = refs[3 + n_in :]
    if role == "last":
        rank_ref, _, _, out, acc1, acc2, back, rows_out, out_sem = refs[:9]
        refs = refs[9:]
    elif role == "next":
        acc1, acc2 = refs[2:4]
        refs = refs[4:]
    else:
        acc1, acc2 = refs[:2]
        refs = refs[2:]
        acc1[...] = jnp.zeros(acc1.shape, F32)
        acc2[...] = jnp.zeros(acc2.shape, F32)
    roll_s, stage0, stage1, weights, c_lo, c_hi, squares = refs
    row_i = lax.broadcasted_iota(jnp.int32, (RC, PS), 0).astype(F32)
    for p, (which, index, dy, dz) in enumerate(pencils):
        if dy != 0 and not shift_here:
            shift_copy.wait()
            shift_here = True
        start = 15 if dy == 0 else lax.rem(shift[0 if dy < 0 else 1] + 15, 16)
        rolled = []
        for f in range(4):
            value = inputs[which][index, f]
            for half in range(2):
                part = value[:, half * 128 : half * 128 + 128]
                for copy in range(3):
                    roll_s[p, 2 * f + half, copy * 16 : copy * 16 + 16, :] = part
            rolled.append(
                jnp.concatenate([roll_s[p, 2 * f, pl.ds(start, RC), :], roll_s[p, 2 * f + 1, pl.ds(start, RC), :]], 1)
            )
        y, x, z, m = rolled
        y = y + float(dy)
        z = z + float(dz)
        x = x + (row_i - 9.0)
        live = (m > 0.0) & (row_i < 18.0)
        cube = jnp.where(live, m, 1.0) * (16.0 / 3.141592653589793)
        c = jnp.where(live, jnp.exp2(jnp.log2(cube) * (1.0 / 3.0)), 0.0)
        w = c * c * 16.0
        norm = w * (y * y + x * x + z * z)
        w2 = w * -2.0
        py, pz, px, pw, pn = pieces(y * w2), pieces(z * w2), pieces(x * w2), pieces(w), pieces(norm)
        features = [py[b] for _, b in SHORT] + [pz[b] for _, b in SHORT] + [px[b] for _, b in FULL] + [pw[b] for _, b in FULL]
        features = features + list(pn) + [jnp.zeros((RC, PS), F32)]
        for k in range(KD):
            stage0[p, pl.ds(k, RC, stride=STRIDE), :] = features[k][:, 0:128]
            stage1[p, pl.ds(k, RC, stride=STRIDE), :] = features[k][:, 128:256]
        c_lo[pl.ds(p * RC, RC), :] = c[:, 0:128]
        c_hi[pl.ds(p * RC, RC), :] = c[:, 128:256]
        for r in range(RC):
            if r < 18 or r == 23:
                weights[p * RC + r, :, 0:128] = stage0[p, r * STRIDE : r * STRIDE + KD, :].astype(BF16)
                weights[p * RC + r, :, 128:256] = stage1[p, r * STRIDE : r * STRIDE + KD, :].astype(BF16)

    def decode(i):
        return pl.multiple_of(table[i], 16), [table[i + ITEMS * field] for field in fields]

    def multiply(i, slot):
        at, sources = decode(i)
        lhs = targets[pl.ds(at, BLOCK), :]
        for n, source in enumerate(sources):
            slot[:, 256 * n : 256 * n + 256] = dot(lhs, weights[source])

    def consume(i, slot):
        at, sources = decode(i)
        cs = [ref[pl.ds(source, 8, stride=0), :] for source in sources for ref in (c_lo, c_hi)]
        for g in range(BLOCK // 8):
            sum1 = acc1[pl.ds(at + 8 * g, 8), :]
            sum2 = acc2[pl.ds(at + 8 * g, 8), :]
            for t, scale in enumerate(cs):
                square = jnp.maximum(slot[8 * g : 8 * g + 8, 128 * t : 128 * t + 128], 1e-30)
                root = square * lax.rsqrt(square)
                inner = scale - root
                outer = jnp.maximum(inner + scale, 0.0)
                inner = jnp.maximum(inner, 0.0)
                sum1 = sum1 + outer * outer * outer
                sum2 = sum2 + inner * inner * inner
            acc1[pl.ds(at + 8 * g, 8), :] = sum1
            acc2[pl.ds(at + 8 * g, 8), :] = sum2

    if not shift_here:
        shift_copy.wait()
    table_copy.wait()
    count = table[META]
    for k in range(group):
        multiply(k, squares.at[k])

    def step(it, carry):
        i = it * group
        for k in range(group):
            consume(i + k, squares.at[k])
        for k in range(group):
            multiply(i + group + k, squares.at[k])
        return carry

    lax.fori_loop(0, (count + group - 1) // group, step, 0)

    if role == "last":
        unsort(table, acc1, acc2, back, rank_ref, rows_out, out, out_sem)


def unsort(table, acc1, acc2, back, rank_ref, rows_out, out, out_sem):
    for q in range(4):

        def place_of(c, q=q):
            at = META + 128 + q * 16 + c
            return table[at], table[at + 64], table[at + 128]

        @pl.when(table[META + 384 + q] <= MOVE)
        def _():
            for c in range(16):
                target, _, source = place_of(c)
                value = acc1[pl.ds(source, MOVE), :] - 4.0 * acc2[pl.ds(source, MOVE), :]
                back[c, pl.ds(target, MOVE), :] = value

        @pl.when(table[META + 384 + q] > MOVE)
        def _():
            def fetch(c, carry):
                target, length, source = place_of(c)

                def chunk(i, carry):
                    value = acc1[pl.ds(source + 64 * i, 64), :] - 4.0 * acc2[pl.ds(source + 64 * i, 64), :]
                    back[c, pl.ds(target + 64 * i, 64), :] = value
                    return carry

                return lax.fori_loop(0, (length + 63) // 64, chunk, carry)

            lax.fori_loop(0, 16, fetch, 0)

    row_f = lax.broadcasted_iota(jnp.int32, (PS, 128), 0).astype(F32)
    ones = jnp.ones((256, 128), BF16)
    for c in range(16):
        value = back[c, 0:PS, :]
        high = value.astype(BF16)
        low = (value - high.astype(F32)).astype(BF16)
        sums = dot(jnp.concatenate([high, low], 1), ones)
        for half in range(2):
            lanes = slice(128 * half, 128 * half + 128)
            mine = row_f == rank_ref[c : c + 1, lanes]
            rows_out[0, c, :, lanes] = jnp.sum(jnp.where(mine, sums, 0.0), 0, keepdims=True)
    copy = pltpu.make_async_copy(rows_out, out, out_sem)
    copy.start()
    copy.wait()


VMEM_SPEC = pl.BlockSpec(memory_space=pltpu.VMEM)
HBM_SPEC = pl.BlockSpec(memory_space=pl.ANY)


def prepare(data, interpret=False):
    return pl.pallas_call(
        prep_kernel,
        out_shape=(
            jax.ShapeDtypeStruct((ROWS, KD), BF16),
            jax.ShapeDtypeStruct((NX, PS), F32),
            jax.ShapeDtypeStruct((24, 128), jnp.int32),
        ),
        in_specs=[VMEM_SPEC],
        out_specs=[VMEM_SPEC] * 3,
        scratch_shapes=[
            pltpu.VMEM((16 * STRIDE, 128), F32),
            pltpu.VMEM((16 * STRIDE, 128), F32),
            pltpu.VMEM((16, PS + MOVE, KD), F32),
            pltpu.VMEM((ROWS, KD), F32),
            pltpu.VMEM((24, 128), jnp.int32),
            pltpu.SMEM((24, 128), jnp.int32),
            pltpu.SemaphoreType.DMA,
        ],
        compiler_params=pltpu.CompilerParams(vmem_limit_bytes=40 << 20),
        interpret=interpret,
        name="prepare",
    )(data)


def pair_sums(pencils, fields, group, role, table, shift, inputs, targets, rest, interpret=False):
    n = len(pencils)
    out_shape = [jax.ShapeDtypeStruct((ROWS, 128), F32)] * 2
    out_specs = [VMEM_SPEC] * 2
    first_in, first_out = len(inputs) + 3, 0
    scratch = [
        pltpu.VMEM((n, 8, 48, 128), F32),
        pltpu.VMEM((n, RC * STRIDE, 128), F32),
        pltpu.VMEM((n, RC * STRIDE, 128), F32),
        pltpu.VMEM((n * RC, KD, PS), BF16),
        pltpu.VMEM((n * RC, 128), F32),
        pltpu.VMEM((n * RC, 128), F32),
        pltpu.VMEM((group, BLOCK, PS * len(fields)), F32),
    ]
    if role == "last":
        out_shape = [jax.ShapeDtypeStruct((1, NX, 1, PS), F32)] + out_shape
        first_in, first_out = first_in + 1, 1
        out_specs = [HBM_SPEC] + out_specs
        scratch = [pltpu.VMEM((NX, PS + MOVE, 128), F32), pltpu.VMEM((1, NX, 1, PS), F32), pltpu.SemaphoreType.DMA] + scratch
    scratch = scratch + [
        pltpu.SMEM((24 * 128,), jnp.int32),
        pltpu.SMEM((2,), jnp.int32),
        pltpu.SemaphoreType.DMA,
        pltpu.SemaphoreType.DMA,
    ]
    aliases = {} if role == "first" else {first_in: first_out, first_in + 1: first_out + 1}
    return pl.pallas_call(
        functools.partial(pair_kernel, pencils, fields, group, len(inputs), role),
        out_shape=out_shape,
        in_specs=[VMEM_SPEC] * (len(inputs) + 3 + len(rest)),
        out_specs=out_specs,
        scratch_shapes=scratch,
        input_output_aliases=aliases,
        compiler_params=pltpu.CompilerParams(vmem_limit_bytes=40 << 20),
        interpret=interpret,
    )(table, shift, *inputs, targets, *rest)


OWN = ((0, 0, 0, 0),)
SIDE = ((0, 0, -1, 0), (1, 0, 1, 0))
FAR = ((0, 0, 0, -1), (1, 0, 0, 1), (0, 1, -1, -1), (1, 1, -1, 1), (0, 2, 1, -1), (1, 2, 1, 1))


def own_sums(table, shift, data, targets):
    return pair_sums(OWN, (1,), 16, "first", table, shift, [data[None]], targets, [])


def side_sums(table, shift, below, above, targets, sums):
    return pair_sums(SIDE, (2,), 16, "next", table, shift, [below[None], above[None]], targets, sums)


def far_sums(table, shift, low, high, targets, rank, sums):
    return pair_sums(FAR, (3, 4), 8, "last", table, shift, [low, high], targets, [rank, *sums])[0]


def ring(axis, distance):
    count = lax.axis_size(axis)
    return [(i, (i + distance) % count) for i in range(count)]


def shards(positions, masses, counts, shear_offset):
    slot_index = lax.broadcasted_iota(jnp.int32, masses.shape, 3)
    weight = jnp.where(slot_index < counts[..., None], masses, jnp.float32(0.0))
    data = jnp.concatenate([positions, weight[None]], 0).reshape(4, NX, PS)
    index = lax.axis_index("shear")
    offset = shear_offset[0]
    shift = jnp.stack([
        jnp.where(index == 0, NX - offset, 0),
        jnp.where(index == lax.axis_size("shear") - 1, offset, 0),
    ]).astype(jnp.int32)
    n_rows = lax.axis_size("shear")
    half = n_rows // 2
    ends = [(i, (i + 1) % n_rows) for i in (half - 1, n_rows - 1)]
    inner = [(i, i + 1) for i in range(n_rows) if (i, (i + 1) % n_rows) not in ends]
    distant = lax.ppermute(data, "shear", ends + [(j, i) for i, j in ends])
    below = lax.ppermute(data, "shear", inner)
    above = lax.ppermute(data, "shear", [(j, i) for i, j in inner])
    targets, rank, table = prepare(data)
    table = table.reshape(-1)
    sums = own_sums(table, shift, data, targets)
    below = jnp.where(lax.rem(index, half) == 0, distant, below)
    above = jnp.where(lax.rem(index, half) == half - 1, distant, above)
    rows = jnp.stack([data, below, above])
    rows, targets, rank, table, shift, sums = lax.optimization_barrier((rows, targets, rank, table, shift, sums))
    low = lax.ppermute(rows, "cross", ring("cross", 1))
    high = lax.ppermute(rows, "cross", ring("cross", -1))
    sums = side_sums(table, shift, rows[1], rows[2], targets, sums)
    density = far_sums(table, shift, low, high, targets, rank, sums)
    return density


def solution(mesh):
    in_specs = (
        P(None, "shear", None, "cross", None),
        P("shear", None, "cross", None),
        P("shear", None, "cross"),
        P(),
    )
    out_specs = P("shear", None, "cross", None)
    return jax.shard_map(shards, mesh=mesh, in_specs=in_specs, out_specs=out_specs, check_vma=False)
```

```python
import functools

import jax
import jax.numpy as jnp
from jax import lax
from jax.experimental import pallas as pl
from jax.experimental.pallas import tpu as pltpu
from jax.sharding import PartitionSpec as P


NX = 16
PS = 256
ROWS = 4480
NULL_ROW = 4416
BLOCK = 32
GAP = 48
MOVE = 96
RC = 24
STRIDE = 33
KD = 32
ITEMS = 512
META = 5 * ITEMS
F32 = jnp.float32
BF16 = jnp.bfloat16

FULL = [(0, 0), (0, 1), (0, 2), (1, 0), (1, 1), (1, 2), (2, 0), (2, 1)]
SHORT = [(0, 0), (0, 1), (0, 2), (1, 0), (1, 1), (2, 0)]


def pieces(value):
    first = value.astype(BF16).astype(F32)
    rest = value - first
    second = rest.astype(BF16).astype(F32)
    return first, second, rest - second


def dot(a, b, dims=((1,), (0,))):
    return lax.dot_general(a, b, (dims, ((), ())), preferred_element_type=F32)


def steps(value, width, most):
    return sum((value >= width * (i + 1)).astype(jnp.int32) for i in range(most))


def prep_kernel(data, t_out, rank_out, list_out, feat0, feat1, sorted_s, t_s, meta_v, meta_s, sem):
    y, x, z, m = data[0], data[1], data[2], data[3]
    valid = m > 0.0
    one = jnp.float32(1.0)
    nil = jnp.float32(0.0)
    code = jnp.where(y >= 0.5, 4.0, 0.0) + jnp.where(z >= 0.5, 2.0, 0.0) + jnp.where(x >= 0.5, 1.0, 0.0)
    code = jnp.where(valid, code, 9.0)
    masks = [jnp.where(code == float(b), one, nil) for b in range(8)]
    stacked = jnp.concatenate(masks, 0).astype(BF16)
    row_i = lax.broadcasted_iota(jnp.int32, (PS, PS), 0)
    lane_i = lax.broadcasted_iota(jnp.int32, (PS, PS), 1)
    upper = jnp.where(row_i <= lane_i, one, nil).astype(BF16)
    running = dot(stacked, upper)
    total = dot(stacked, jnp.ones((PS, 128), BF16))
    begin = jnp.zeros((16, 128), F32)
    rank = jnp.zeros((16, PS), F32)
    for b in range(8):
        wide = jnp.concatenate([begin, begin], 1)
        rank = rank + masks[b] * (wide + running[b * 16 : b * 16 + 16] - 1.0)
        begin = begin + total[b * 16 : b * 16 + 16]
    rank = jnp.where(valid, rank, -1.0)
    rank_out[...] = rank

    g = lax.broadcasted_iota(jnp.int32, (200, 128), 0)
    j = lax.broadcasted_iota(jnp.int32, (200, 128), 1)
    kind = steps(g, 96, 2)
    g = g - 96 * kind
    group_q = steps(g, RC, 3)
    group_x = g - RC * group_q - 1
    limit = jnp.where(kind == 0, 2 * group_x - 1, jnp.where(group_x > 16, 0, 2 * group_x + 3))
    limit = jnp.where((kind == 0) & (group_x > 16), 0, limit)
    limit = jnp.where(kind == 2, 32, limit)
    group_q = jnp.where(kind == 2, g, group_q)
    spot = 2 * (j & 15) + ((j >> 4) & 1)
    counted = ((j >> 5) == group_q) & (spot < limit)
    columns = dot(jnp.where(counted, one, nil).astype(BF16), total.astype(BF16))
    base = [jnp.zeros((1, 128), F32)]
    for q in range(3):
        end = base[q] + columns[192 + q : 193 + q] + float(GAP + 15)
        base.append(jnp.floor(end * 0.0625) * 16.0)
    base_col = jnp.concatenate([jnp.broadcast_to(b, (RC, 128)) for b in base], 0)
    low, high = columns[0:96], columns[96:192]
    first = jnp.floor((low + base_col) * 0.0625) * 16.0
    n_blocks = jnp.floor((high + base_col - first + float(BLOCK - 1)) * (1.0 / BLOCK))
    n_blocks = jnp.where(high > low, n_blocks, 0.0)
    gi = lax.broadcasted_iota(jnp.int32, (96, 96), 0)
    gj = lax.broadcasted_iota(jnp.int32, (96, 96), 1)
    before = dot(jnp.where(gj < gi, one, nil).astype(BF16), n_blocks.astype(BF16))
    group_r = lax.broadcasted_iota(jnp.int32, (96, 128), 0)
    group_q = steps(group_r, RC, 3)
    cell_r = group_r - group_q * RC
    fields = [
        cell_r,
        cell_r + RC * (group_q >> 1),
        cell_r + RC * (group_q & 1),
        cell_r + RC * (2 + group_q),
    ]
    lane96 = lax.broadcasted_iota(jnp.int32, (96, 128), 1).astype(F32)
    away = [lane96 + float(128 * t) - before for t in range(4)]
    inside = [(v >= 0.0) & (v < n_blocks) for v in away]
    out_rows = []
    for t in range(4):
        entry = first + away[t] * float(BLOCK) - float(NULL_ROW)
        out_rows.append(jnp.sum(jnp.where(inside[t], entry, 0.0), 0, keepdims=True) + float(NULL_ROW))
    for field in fields:
        entry = field.astype(F32) - float(RC - 1)
        for t in range(4):
            out_rows.append(jnp.sum(jnp.where(inside[t], entry, 0.0), 0, keepdims=True) + float(RC - 1))
    out_rows.append(before[95:96] + n_blocks[95:96])
    total_row = dot(jnp.ones((8, PS), BF16), stacked, ((1,), (1,)))
    j = lax.broadcasted_iota(jnp.int32, (128, 256), 0)
    k = lax.broadcasted_iota(jnp.int32, (128, 256), 1)
    quad, kind, goal = j >> 5, k >> 6, (k & 63) >> 4
    same, earlier = (j & 15) == (k & 15), (j & 15) < (k & 15)
    counted = ((kind == 0) & same & (quad < goal)) | ((kind == 1) & same & (quad == goal))
    counted = counted | ((kind == 2) & earlier & (quad == goal))
    meta = dot(total_row.astype(BF16), jnp.where(counted, one, nil).astype(BF16))
    lane1 = lax.broadcasted_iota(jnp.int32, (1, 128), 1)
    base_lane = jnp.where(lane1 < 16, base[0], jnp.where(lane1 < 32, base[1], jnp.where(lane1 < 48, base[2], base[3])))
    out_rows.append(meta[0:1, 0:128])
    out_rows.append(meta[0:1, 128:256] + base_lane)
    longest = jnp.where(lane1 >= 64, meta[0:1, 0:128], 0.0)
    flags = jnp.zeros((1, 128), F32)
    for q in range(4):
        top = jnp.max(jnp.where((lane1 >= 64 + 16 * q) & (lane1 < 80 + 16 * q), longest, 0.0), 1, keepdims=True)
        flags = jnp.where(lane1 == q, top, flags)
    out_rows.append(flags)
    table = jnp.concatenate(out_rows, 0).astype(jnp.int32)
    list_out[...] = table
    meta_v[...] = table
    copy = pltpu.make_async_copy(meta_v, meta_s, sem)
    copy.start()

    cell_i = lax.broadcasted_iota(jnp.int32, (16, PS), 0).astype(F32)
    xg = x + (cell_i - 8.0)
    norm = y * y + xg * xg + z * z
    py, pz, px, pn = pieces(y), pieces(z), pieces(xg), pieces(norm)
    features = [py[a] for a, _ in SHORT] + [pz[a] for a, _ in SHORT] + [px[a] for a, _ in FULL] + [pn[a] for a, _ in FULL]
    ones = jnp.ones((16, PS), F32)
    features = features + [ones, ones, ones, jnp.zeros((16, PS), F32)]
    for k in range(KD):
        feat0[pl.ds(k, 16, stride=STRIDE), :] = features[k][:, 0:128]
        feat1[pl.ds(k, 16, stride=STRIDE), :] = features[k][:, 128:256]
    t_s[...] = jnp.zeros(t_s.shape, F32)
    row_b = row_i.astype(F32).astype(BF16)
    for c in range(16):
        place = jnp.where(row_b == rank[c : c + 1].astype(BF16), jnp.bfloat16(1.0), jnp.bfloat16(0.0))
        both = jnp.concatenate([feat0[c * STRIDE : c * STRIDE + KD, :], feat1[c * STRIDE : c * STRIDE + KD, :]], 1)
        sorted_s[c, 0:PS, :] = dot(place, both.astype(BF16), ((1,), (1,)))
        sorted_s[c, PS : PS + MOVE, :] = jnp.zeros((MOVE, KD), F32)
    copy.wait()
    for q in range(4):

        def place_of(c, q=q):
            return meta_s[21, q * 16 + c], meta_s[21, 64 + q * 16 + c], meta_s[22, q * 16 + c]

        @pl.when(meta_s[23, q] <= MOVE)
        def _():
            for c in range(16):
                source, _, target = place_of(c)
                t_s[pl.ds(target, MOVE), :] = sorted_s[c, pl.ds(source, MOVE), :]

        @pl.when(meta_s[23, q] > MOVE)
        def _():
            def append(c, carry):
                source, count, target = place_of(c)

                def chunk(i, carry):
                    t_s[pl.ds(target + 64 * i, 64), :] = sorted_s[c, pl.ds(source + 64 * i, 64), :]
                    return carry

                return lax.fori_loop(0, (count + 63) // 64, chunk, carry)

            lax.fori_loop(0, 16, append, 0)

    t_out[...] = t_s[...].astype(BF16)


def pair_kernel(pencils, fields, group, n_in, role, *refs):
    inputs = refs[2 : 2 + n_in]
    table, shift, table_sem, shift_sem = refs[-4:]
    table_copy = pltpu.make_async_copy(refs[0], table, table_sem)
    shift_copy = pltpu.make_async_copy(refs[1], shift, shift_sem)
    shift_copy.start()
    table_copy.start()
    shift_here = False
    refs = refs[:-4]
    targets = refs[2 + n_in]
    refs = refs[3 + n_in :]
    if role == "last":
        rank_ref, _, _, out, acc1, acc2, back, rows_out, out_sem = refs[:9]
        refs = refs[9:]
    elif role == "next":
        acc1, acc2 = refs[2:4]
        refs = refs[4:]
    else:
        acc1, acc2 = refs[:2]
        refs = refs[2:]
        acc1[...] = jnp.zeros(acc1.shape, F32)
        acc2[...] = jnp.zeros(acc2.shape, F32)
    roll_s, stage0, stage1, weights, c_lo, c_hi, squares = refs
    row_i = lax.broadcasted_iota(jnp.int32, (RC, PS), 0).astype(F32)
    for p, (which, index, dy, dz) in enumerate(pencils):
        if dy != 0 and not shift_here:
            shift_copy.wait()
            shift_here = True
        start = 15 if dy == 0 else lax.rem(shift[0 if dy < 0 else 1] + 15, 16)
        rolled = []
        for f in range(4):
            value = inputs[which][index, f]
            for half in range(2):
                part = value[:, half * 128 : half * 128 + 128]
                for copy in range(3):
                    roll_s[p, 2 * f + half, copy * 16 : copy * 16 + 16, :] = part
            rolled.append(
                jnp.concatenate([roll_s[p, 2 * f, pl.ds(start, RC), :], roll_s[p, 2 * f + 1, pl.ds(start, RC), :]], 1)
            )
        y, x, z, m = rolled
        y = y + float(dy)
        z = z + float(dz)
        x = x + (row_i - 9.0)
        live = (m > 0.0) & (row_i < 18.0)
        cube = jnp.where(live, m, 1.0) * (16.0 / 3.141592653589793)
        c = jnp.where(live, jnp.exp2(jnp.log2(cube) * (1.0 / 3.0)), 0.0)
        w = c * c * 16.0
        norm = w * (y * y + x * x + z * z)
        w2 = w * -2.0
        py, pz, px, pw, pn = pieces(y * w2), pieces(z * w2), pieces(x * w2), pieces(w), pieces(norm)
        features = [py[b] for _, b in SHORT] + [pz[b] for _, b in SHORT] + [px[b] for _, b in FULL] + [pw[b] for _, b in FULL]
        features = features + list(pn) + [jnp.zeros((RC, PS), F32)]
        for k in range(KD):
            stage0[p, pl.ds(k, RC, stride=STRIDE), :] = features[k][:, 0:128]
            stage1[p, pl.ds(k, RC, stride=STRIDE), :] = features[k][:, 128:256]
        c_lo[pl.ds(p * RC, RC), :] = c[:, 0:128]
        c_hi[pl.ds(p * RC, RC), :] = c[:, 128:256]
        for r in range(RC):
            if r < 18 or r == 23:
                weights[p * RC + r, :, 0:128] = stage0[p, r * STRIDE : r * STRIDE + KD, :].astype(BF16)
                weights[p * RC + r, :, 128:256] = stage1[p, r * STRIDE : r * STRIDE + KD, :].astype(BF16)

    def decode(i):
        return pl.multiple_of(table[i], 16), [table[i + ITEMS * field] for field in fields]

    def multiply(i, slot):
        at, sources = decode(i)
        lhs = targets[pl.ds(at, BLOCK), :]
        for n, source in enumerate(sources):
            slot[:, 256 * n : 256 * n + 256] = dot(lhs, weights[source])

    def consume(i, slot):
        at, sources = decode(i)
        cs = [ref[pl.ds(source, 8, stride=0), :] for source in sources for ref in (c_lo, c_hi)]
        for g in range(BLOCK // 8):
            sum1 = acc1[pl.ds(at + 8 * g, 8), :]
            sum2 = acc2[pl.ds(at + 8 * g, 8), :]
            for t, scale in enumerate(cs):
                square = jnp.maximum(slot[8 * g : 8 * g + 8, 128 * t : 128 * t + 128], 1e-30)
                root = square * lax.rsqrt(square)
                inner = scale - root
                outer = jnp.maximum(inner + scale, 0.0)
                inner = jnp.maximum(inner, 0.0)
                sum1 = sum1 + outer * outer * outer
                sum2 = sum2 + inner * inner * inner
            acc1[pl.ds(at + 8 * g, 8), :] = sum1
            acc2[pl.ds(at + 8 * g, 8), :] = sum2

    if not shift_here:
        shift_copy.wait()
    table_copy.wait()
    count = table[META]
    for k in range(group):
        multiply(k, squares.at[k])

    def step(it, carry):
        i = it * group
        for k in range(group):
            consume(i + k, squares.at[k])
        for k in range(group):
            multiply(i + group + k, squares.at[k])
        return carry

    lax.fori_loop(0, (count + group - 1) // group, step, 0)

    if role == "last":
        unsort(table, acc1, acc2, back, rank_ref, rows_out, out, out_sem)


def unsort(table, acc1, acc2, back, rank_ref, rows_out, out, out_sem):
    for q in range(4):

        def place_of(c, q=q):
            at = META + 128 + q * 16 + c
            return table[at], table[at + 64], table[at + 128]

        @pl.when(table[META + 384 + q] <= MOVE)
        def _():
            for c in range(16):
                target, _, source = place_of(c)
                value = acc1[pl.ds(source, MOVE), :] - 4.0 * acc2[pl.ds(source, MOVE), :]
                back[c, pl.ds(target, MOVE), :] = value

        @pl.when(table[META + 384 + q] > MOVE)
        def _():
            def fetch(c, carry):
                target, length, source = place_of(c)

                def chunk(i, carry):
                    value = acc1[pl.ds(source + 64 * i, 64), :] - 4.0 * acc2[pl.ds(source + 64 * i, 64), :]
                    back[c, pl.ds(target + 64 * i, 64), :] = value
                    return carry

                return lax.fori_loop(0, (length + 63) // 64, chunk, carry)

            lax.fori_loop(0, 16, fetch, 0)

    row_f = lax.broadcasted_iota(jnp.int32, (PS, 128), 0).astype(F32)
    ones = jnp.ones((256, 128), BF16)
    for c in range(16):
        value = back[c, 0:PS, :]
        high = value.astype(BF16)
        low = (value - high.astype(F32)).astype(BF16)
        sums = dot(jnp.concatenate([high, low], 1), ones)
        for half in range(2):
            lanes = slice(128 * half, 128 * half + 128)
            mine = row_f == rank_ref[c : c + 1, lanes]
            rows_out[0, c, :, lanes] = jnp.sum(jnp.where(mine, sums, 0.0), 0, keepdims=True)
    copy = pltpu.make_async_copy(rows_out, out, out_sem)
    copy.start()
    copy.wait()


VMEM_SPEC = pl.BlockSpec(memory_space=pltpu.VMEM)
HBM_SPEC = pl.BlockSpec(memory_space=pl.ANY)


def gated(kernel, first_row, skip, count):
    def run(*refs):
        here = lax.axis_index("shear") == 0

        @pl.when(here if first_row else jnp.logical_not(here))
        def _():
            kernel(*refs[:skip], *refs[skip + count :])

    return run


def prepare(data, old=()):
    return pl.pallas_call(
        gated(prep_kernel, not old, 1, len(old)),
        out_shape=(
            jax.ShapeDtypeStruct((ROWS, KD), BF16),
            jax.ShapeDtypeStruct((NX, PS), F32),
            jax.ShapeDtypeStruct((24, 128), jnp.int32),
        ),
        in_specs=[VMEM_SPEC] * (1 + len(old)),
        out_specs=[VMEM_SPEC] * 3,
        scratch_shapes=[
            pltpu.VMEM((16 * STRIDE, 128), F32),
            pltpu.VMEM((16 * STRIDE, 128), F32),
            pltpu.VMEM((16, PS + MOVE, KD), F32),
            pltpu.VMEM((ROWS, KD), F32),
            pltpu.VMEM((24, 128), jnp.int32),
            pltpu.SMEM((24, 128), jnp.int32),
            pltpu.SemaphoreType.DMA,
        ],
        input_output_aliases={1 + i: i for i in range(len(old))},
        compiler_params=pltpu.CompilerParams(vmem_limit_bytes=16 << 20),
        name="prepare_rest" if old else "prepare_first",
    )(data, *old)


def pair_sums(pencils, fields, group, role, table, shift, inputs, targets, rest, interpret=False):
    n = len(pencils)
    out_shape = [jax.ShapeDtypeStruct((ROWS, 128), F32)] * 2
    out_specs = [VMEM_SPEC] * 2
    first_in, first_out = len(inputs) + 3, 0
    scratch = [
        pltpu.VMEM((n, 8, 48, 128), F32),
        pltpu.VMEM((n, RC * STRIDE, 128), F32),
        pltpu.VMEM((n, RC * STRIDE, 128), F32),
        pltpu.VMEM((n * RC, KD, PS), BF16),
        pltpu.VMEM((n * RC, 128), F32),
        pltpu.VMEM((n * RC, 128), F32),
        pltpu.VMEM((group, BLOCK, PS * len(fields)), F32),
    ]
    if role == "last":
        out_shape = [jax.ShapeDtypeStruct((1, NX, 1, PS), F32)] + out_shape
        first_in, first_out = first_in + 1, 1
        out_specs = [HBM_SPEC] + out_specs
        scratch = [pltpu.VMEM((NX, PS + MOVE, 128), F32), pltpu.VMEM((1, NX, 1, PS), F32), pltpu.SemaphoreType.DMA] + scratch
    scratch = scratch + [
        pltpu.SMEM((24 * 128,), jnp.int32),
        pltpu.SMEM((2,), jnp.int32),
        pltpu.SemaphoreType.DMA,
        pltpu.SemaphoreType.DMA,
    ]
    kernel = functools.partial(pair_kernel, pencils, fields, group, len(inputs), role)
    if role == "first":
        kernel = gated(kernel, not rest, first_in, len(rest))
    aliases = {} if not rest else {first_in: first_out, first_in + 1: first_out + 1}
    return pl.pallas_call(
        kernel,
        out_shape=out_shape,
        in_specs=[VMEM_SPEC] * (len(inputs) + 3 + len(rest)),
        out_specs=out_specs,
        scratch_shapes=scratch,
        input_output_aliases=aliases,
        compiler_params=pltpu.CompilerParams(vmem_limit_bytes=20 << 20),
        interpret=interpret,
    )(table, shift, *inputs, targets, *rest)


OWN = ((0, 0, 0, 0),)
SIDE = ((0, 0, -1, 0), (1, 0, 1, 0))
FAR = ((0, 0, 0, -1), (1, 0, 0, 1), (0, 1, -1, -1), (1, 1, -1, 1), (0, 2, 1, -1), (1, 2, 1, 1))


def own_sums(table, shift, data, targets, old=()):
    return pair_sums(OWN, (1,), 16, "first", table, shift, [data[None]], targets, old)


def side_sums(table, shift, below, above, targets, sums):
    return pair_sums(SIDE, (2,), 16, "next", table, shift, [below[None], above[None]], targets, sums)


def far_sums(table, shift, low, high, targets, rank, sums):
    return pair_sums(FAR, (3, 4), 8, "last", table, shift, [low, high], targets, [rank, *sums])[0]


def ring(axis, distance):
    count = lax.axis_size(axis)
    return [(i, (i + distance) % count) for i in range(count)]


def shards(positions, masses, counts, shear_offset):
    slot_index = lax.broadcasted_iota(jnp.int32, masses.shape, 3)
    weight = jnp.where(slot_index < counts[..., None], masses, jnp.float32(0.0))
    data = jnp.concatenate([positions, weight[None]], 0).reshape(4, NX, PS)
    index = lax.axis_index("shear")
    offset = shear_offset[0]
    shift = jnp.stack([
        jnp.where(index == 0, NX - offset, 0),
        jnp.where(index == lax.axis_size("shear") - 1, offset, 0),
    ]).astype(jnp.int32)
    n_rows = lax.axis_size("shear")
    half = n_rows // 2
    inner = [(i, (i + 1) % n_rows) for i in range(n_rows) if i != half - 1]
    middle = lax.ppermute(data, "shear", [(half - 1, half), (half, half - 1)])
    below = lax.ppermute(data, "shear", inner)
    first = prepare(data)
    first_sums = own_sums(first[2].reshape(-1), shift, data, first[0])
    data, first, first_sums = lax.optimization_barrier((data, tuple(first), tuple(first_sums)))
    above = lax.ppermute(data, "shear", [(j, i) for i, j in inner])
    targets, rank, table = prepare(data, first)
    table = table.reshape(-1)
    sums = own_sums(table, shift, data, targets, first_sums)
    below = jnp.where(index == half, middle, below)
    above = jnp.where(index == half - 1, middle, above)
    rows = jnp.stack([data, below, above])
    rows, targets, rank, table, shift, sums = lax.optimization_barrier((rows, targets, rank, table, shift, sums))
    low = lax.ppermute(rows, "cross", ring("cross", 1))
    high = lax.ppermute(rows, "cross", ring("cross", -1))
    sums = side_sums(table, shift, rows[1], rows[2], targets, sums)
    density = far_sums(table, shift, low, high, targets, rank, sums)
    return density


def solution(mesh):
    in_specs = (
        P(None, "shear", None, "cross", None),
        P("shear", None, "cross", None),
        P("shear", None, "cross"),
        P(),
    )
    out_specs = P("shear", None, "cross", None)
    return jax.shard_map(shards, mesh=mesh, in_specs=in_specs, out_specs=out_specs, check_vma=False)
```

```python
import functools

import jax
import jax.numpy as jnp
from jax import lax
from jax.experimental import pallas as pl
from jax.experimental.pallas import tpu as pltpu
from jax.sharding import PartitionSpec as P


NX = 16
PS = 256
ROWS = 4480
NULL_ROW = 4416
BLOCK = 32
GAP = 48
MOVE = 96
RC = 24
STRIDE = 33
KD = 32
ITEMS = 512
META = 5 * ITEMS
F32 = jnp.float32
BF16 = jnp.bfloat16

FULL = [(0, 0), (0, 1), (0, 2), (1, 0), (1, 1), (1, 2), (2, 0), (2, 1)]
SHORT = [(0, 0), (0, 1), (0, 2), (1, 0), (1, 1), (2, 0)]


def pieces(value):
    first = value.astype(BF16).astype(F32)
    rest = value - first
    second = rest.astype(BF16).astype(F32)
    return first, second, rest - second


def dot(a, b, dims=((1,), (0,))):
    return lax.dot_general(a, b, (dims, ((), ())), preferred_element_type=F32)


def steps(value, width, most):
    return sum((value >= width * (i + 1)).astype(jnp.int32) for i in range(most))


def prep_kernel(data, t_out, rank_out, list_out, feat0, feat1, sorted_s, t_s, meta_v, meta_s, sem):
    y, x, z, m = data[0], data[1], data[2], data[3]
    valid = m > 0.0
    one = jnp.float32(1.0)
    nil = jnp.float32(0.0)
    code = jnp.where(y >= 0.5, 4.0, 0.0) + jnp.where(z >= 0.5, 2.0, 0.0) + jnp.where(x >= 0.5, 1.0, 0.0)
    code = jnp.where(valid, code, 9.0)
    masks = [jnp.where(code == float(b), one, nil) for b in range(8)]
    stacked = jnp.concatenate(masks, 0).astype(BF16)
    row_i = lax.broadcasted_iota(jnp.int32, (PS, PS), 0)
    lane_i = lax.broadcasted_iota(jnp.int32, (PS, PS), 1)
    upper = jnp.where(row_i <= lane_i, one, nil).astype(BF16)
    running = dot(stacked, upper)
    total = dot(stacked, jnp.ones((PS, 128), BF16))
    begin = jnp.zeros((16, 128), F32)
    rank = jnp.zeros((16, PS), F32)
    for b in range(8):
        wide = jnp.concatenate([begin, begin], 1)
        rank = rank + masks[b] * (wide + running[b * 16 : b * 16 + 16] - 1.0)
        begin = begin + total[b * 16 : b * 16 + 16]
    rank = jnp.where(valid, rank, -1.0)
    rank_out[...] = rank

    g = lax.broadcasted_iota(jnp.int32, (200, 128), 0)
    j = lax.broadcasted_iota(jnp.int32, (200, 128), 1)
    kind = steps(g, 96, 2)
    g = g - 96 * kind
    group_q = steps(g, RC, 3)
    group_x = g - RC * group_q - 1
    limit = jnp.where(kind == 0, 2 * group_x - 1, jnp.where(group_x > 16, 0, 2 * group_x + 3))
    limit = jnp.where((kind == 0) & (group_x > 16), 0, limit)
    limit = jnp.where(kind == 2, 32, limit)
    group_q = jnp.where(kind == 2, g, group_q)
    spot = 2 * (j & 15) + ((j >> 4) & 1)
    counted = ((j >> 5) == group_q) & (spot < limit)
    columns = dot(jnp.where(counted, one, nil).astype(BF16), total.astype(BF16))
    base = [jnp.zeros((1, 128), F32)]
    for q in range(3):
        end = base[q] + columns[192 + q : 193 + q] + float(GAP + 15)
        base.append(jnp.floor(end * 0.0625) * 16.0)
    base_col = jnp.concatenate([jnp.broadcast_to(b, (RC, 128)) for b in base], 0)
    low, high = columns[0:96], columns[96:192]
    first = jnp.floor((low + base_col) * 0.0625) * 16.0
    n_blocks = jnp.floor((high + base_col - first + float(BLOCK - 1)) * (1.0 / BLOCK))
    n_blocks = jnp.where(high > low, n_blocks, 0.0)
    gi = lax.broadcasted_iota(jnp.int32, (96, 96), 0)
    gj = lax.broadcasted_iota(jnp.int32, (96, 96), 1)
    before = dot(jnp.where(gj < gi, one, nil).astype(BF16), n_blocks.astype(BF16))
    group_r = lax.broadcasted_iota(jnp.int32, (96, 128), 0)
    group_q = steps(group_r, RC, 3)
    cell_r = group_r - group_q * RC
    fields = [
        cell_r,
        cell_r + RC * (group_q >> 1),
        cell_r + RC * (group_q & 1),
        cell_r + RC * (2 + group_q),
    ]
    lane96 = lax.broadcasted_iota(jnp.int32, (96, 128), 1).astype(F32)
    away = [lane96 + float(128 * t) - before for t in range(4)]
    inside = [(v >= 0.0) & (v < n_blocks) for v in away]
    out_rows = []
    for t in range(4):
        entry = first + away[t] * float(BLOCK) - float(NULL_ROW)
        out_rows.append(jnp.sum(jnp.where(inside[t], entry, 0.0), 0, keepdims=True) + float(NULL_ROW))
    for field in fields:
        entry = field.astype(F32) - float(RC - 1)
        for t in range(4):
            out_rows.append(jnp.sum(jnp.where(inside[t], entry, 0.0), 0, keepdims=True) + float(RC - 1))
    out_rows.append(before[95:96] + n_blocks[95:96])
    total_row = dot(jnp.ones((8, PS), BF16), stacked, ((1,), (1,)))
    j = lax.broadcasted_iota(jnp.int32, (128, 256), 0)
    k = lax.broadcasted_iota(jnp.int32, (128, 256), 1)
    quad, kind, goal = j >> 5, k >> 6, (k & 63) >> 4
    same, earlier = (j & 15) == (k & 15), (j & 15) < (k & 15)
    counted = ((kind == 0) & same & (quad < goal)) | ((kind == 1) & same & (quad == goal))
    counted = counted | ((kind == 2) & earlier & (quad == goal))
    meta = dot(total_row.astype(BF16), jnp.where(counted, one, nil).astype(BF16))
    lane1 = lax.broadcasted_iota(jnp.int32, (1, 128), 1)
    base_lane = jnp.where(lane1 < 16, base[0], jnp.where(lane1 < 32, base[1], jnp.where(lane1 < 48, base[2], base[3])))
    out_rows.append(meta[0:1, 0:128])
    out_rows.append(meta[0:1, 128:256] + base_lane)
    longest = jnp.where(lane1 >= 64, meta[0:1, 0:128], 0.0)
    flags = jnp.zeros((1, 128), F32)
    for q in range(4):
        top = jnp.max(jnp.where((lane1 >= 64 + 16 * q) & (lane1 < 80 + 16 * q), longest, 0.0), 1, keepdims=True)
        flags = jnp.where(lane1 == q, top, flags)
    out_rows.append(flags)
    table = jnp.concatenate(out_rows, 0).astype(jnp.int32)
    list_out[...] = table
    meta_v[...] = table
    copy = pltpu.make_async_copy(meta_v, meta_s, sem)
    copy.start()

    cell_i = lax.broadcasted_iota(jnp.int32, (16, PS), 0).astype(F32)
    xg = x + (cell_i - 8.0)
    norm = y * y + xg * xg + z * z
    py, pz, px, pn = pieces(y), pieces(z), pieces(xg), pieces(norm)
    features = [py[a] for a, _ in SHORT] + [pz[a] for a, _ in SHORT] + [px[a] for a, _ in FULL] + [pn[a] for a, _ in FULL]
    ones = jnp.ones((16, PS), F32)
    features = features + [ones, ones, ones, jnp.zeros((16, PS), F32)]
    for k in range(KD):
        feat0[pl.ds(k, 16, stride=STRIDE), :] = features[k][:, 0:128]
        feat1[pl.ds(k, 16, stride=STRIDE), :] = features[k][:, 128:256]
    t_s[...] = jnp.zeros(t_s.shape, F32)
    row_b = row_i.astype(F32).astype(BF16)
    for c in range(16):
        place = jnp.where(row_b == rank[c : c + 1].astype(BF16), jnp.bfloat16(1.0), jnp.bfloat16(0.0))
        both = jnp.concatenate([feat0[c * STRIDE : c * STRIDE + KD, :], feat1[c * STRIDE : c * STRIDE + KD, :]], 1)
        sorted_s[c, 0:PS, :] = dot(place, both.astype(BF16), ((1,), (1,)))
        sorted_s[c, PS : PS + MOVE, :] = jnp.zeros((MOVE, KD), F32)
    copy.wait()
    for q in range(4):

        def place_of(c, q=q):
            return meta_s[21, q * 16 + c], meta_s[21, 64 + q * 16 + c], meta_s[22, q * 16 + c]

        @pl.when(meta_s[23, q] <= MOVE)
        def _():
            for c in range(16):
                source, _, target = place_of(c)
                t_s[pl.ds(target, MOVE), :] = sorted_s[c, pl.ds(source, MOVE), :]

        @pl.when(meta_s[23, q] > MOVE)
        def _():
            def append(c, carry):
                source, count, target = place_of(c)

                def chunk(i, carry):
                    t_s[pl.ds(target + 64 * i, 64), :] = sorted_s[c, pl.ds(source + 64 * i, 64), :]
                    return carry

                return lax.fori_loop(0, (count + 63) // 64, chunk, carry)

            lax.fori_loop(0, 16, append, 0)

    t_out[...] = t_s[...].astype(BF16)


def pair_kernel(pencils, fields, group, n_in, role, *refs):
    inputs = refs[2 : 2 + n_in]
    table, shift, table_sem, shift_sem = refs[-4:]
    table_copy = pltpu.make_async_copy(refs[0], table, table_sem)
    shift_copy = pltpu.make_async_copy(refs[1], shift, shift_sem)
    shift_copy.start()
    table_copy.start()
    shift_here = False
    refs = refs[:-4]
    targets = refs[2 + n_in]
    refs = refs[3 + n_in :]
    if role == "last":
        rank_ref, _, _, out, acc1, acc2, back, rows_out, out_sem = refs[:9]
        refs = refs[9:]
    elif role == "next":
        acc1, acc2 = refs[2:4]
        refs = refs[4:]
    else:
        acc1, acc2 = refs[:2]
        refs = refs[2:]
        acc1[...] = jnp.zeros(acc1.shape, F32)
        acc2[...] = jnp.zeros(acc2.shape, F32)
    roll_s, stage0, stage1, weights, c_lo, c_hi, squares = refs
    row_i = lax.broadcasted_iota(jnp.int32, (RC, PS), 0).astype(F32)
    for p, (which, index, dy, dz) in enumerate(pencils):
        if dy != 0 and not shift_here:
            shift_copy.wait()
            shift_here = True
        start = 15 if dy == 0 else lax.rem(shift[0 if dy < 0 else 1] + 15, 16)
        rolled = []
        for f in range(4):
            value = inputs[which][index, f]
            for half in range(2):
                part = value[:, half * 128 : half * 128 + 128]
                for copy in range(3):
                    roll_s[p, 2 * f + half, copy * 16 : copy * 16 + 16, :] = part
            rolled.append(
                jnp.concatenate([roll_s[p, 2 * f, pl.ds(start, RC), :], roll_s[p, 2 * f + 1, pl.ds(start, RC), :]], 1)
            )
        y, x, z, m = rolled
        y = y + float(dy)
        z = z + float(dz)
        x = x + (row_i - 9.0)
        live = (m > 0.0) & (row_i < 18.0)
        cube = jnp.where(live, m, 1.0) * (16.0 / 3.141592653589793)
        c = jnp.where(live, jnp.exp2(jnp.log2(cube) * (1.0 / 3.0)), 0.0)
        w = c * c * 16.0
        norm = w * (y * y + x * x + z * z)
        w2 = w * -2.0
        py, pz, px, pw, pn = pieces(y * w2), pieces(z * w2), pieces(x * w2), pieces(w), pieces(norm)
        features = [py[b] for _, b in SHORT] + [pz[b] for _, b in SHORT] + [px[b] for _, b in FULL] + [pw[b] for _, b in FULL]
        features = features + list(pn) + [jnp.zeros((RC, PS), F32)]
        for k in range(KD):
            stage0[p, pl.ds(k, RC, stride=STRIDE), :] = features[k][:, 0:128]
            stage1[p, pl.ds(k, RC, stride=STRIDE), :] = features[k][:, 128:256]
        c_lo[pl.ds(p * RC, RC), :] = c[:, 0:128]
        c_hi[pl.ds(p * RC, RC), :] = c[:, 128:256]
        for r in range(RC):
            if r < 18 or r == 23:
                weights[p * RC + r, :, 0:128] = stage0[p, r * STRIDE : r * STRIDE + KD, :].astype(BF16)
                weights[p * RC + r, :, 128:256] = stage1[p, r * STRIDE : r * STRIDE + KD, :].astype(BF16)

    def decode(i):
        return pl.multiple_of(table[i], 16), [table[i + ITEMS * field] for field in fields]

    def multiply(i, slot):
        at, sources = decode(i)
        lhs = targets[pl.ds(at, BLOCK), :]
        for n, source in enumerate(sources):
            slot[:, 256 * n : 256 * n + 256] = dot(lhs, weights[source])

    def consume(i, slot):
        at, sources = decode(i)
        cs = [ref[pl.ds(source, 8, stride=0), :] for source in sources for ref in (c_lo, c_hi)]
        for g in range(BLOCK // 8):
            sum1 = acc1[pl.ds(at + 8 * g, 8), :]
            sum2 = acc2[pl.ds(at + 8 * g, 8), :]
            for t, scale in enumerate(cs):
                square = jnp.maximum(slot[8 * g : 8 * g + 8, 128 * t : 128 * t + 128], 1e-30)
                root = square * lax.rsqrt(square)
                inner = scale - root
                outer = jnp.maximum(inner + scale, 0.0)
                inner = jnp.maximum(inner, 0.0)
                sum1 = sum1 + outer * outer * outer
                sum2 = sum2 + inner * inner * inner
            acc1[pl.ds(at + 8 * g, 8), :] = sum1
            acc2[pl.ds(at + 8 * g, 8), :] = sum2

    if not shift_here:
        shift_copy.wait()
    table_copy.wait()
    count = table[META]
    for k in range(group):
        multiply(k, squares.at[k])

    def step(it, carry):
        i = it * group
        for k in range(group):
            consume(i + k, squares.at[k])
        for k in range(group):
            multiply(i + group + k, squares.at[k])
        return carry

    lax.fori_loop(0, (count + group - 1) // group, step, 0)

    if role == "last":
        unsort(table, acc1, acc2, back, rank_ref, rows_out, out, out_sem)


def unsort(table, acc1, acc2, back, rank_ref, rows_out, out, out_sem):
    for q in range(4):

        def place_of(c, q=q):
            at = META + 128 + q * 16 + c
            return table[at], table[at + 64], table[at + 128]

        @pl.when(table[META + 384 + q] <= MOVE)
        def _():
            for c in range(16):
                target, _, source = place_of(c)
                value = acc1[pl.ds(source, MOVE), :] - 4.0 * acc2[pl.ds(source, MOVE), :]
                back[c, pl.ds(target, MOVE), :] = value

        @pl.when(table[META + 384 + q] > MOVE)
        def _():
            def fetch(c, carry):
                target, length, source = place_of(c)

                def chunk(i, carry):
                    value = acc1[pl.ds(source + 64 * i, 64), :] - 4.0 * acc2[pl.ds(source + 64 * i, 64), :]
                    back[c, pl.ds(target + 64 * i, 64), :] = value
                    return carry

                return lax.fori_loop(0, (length + 63) // 64, chunk, carry)

            lax.fori_loop(0, 16, fetch, 0)

    row_f = lax.broadcasted_iota(jnp.int32, (PS, 128), 0).astype(F32)
    ones = jnp.ones((256, 128), BF16)
    for c in range(16):
        value = back[c, 0:PS, :]
        high = value.astype(BF16)
        low = (value - high.astype(F32)).astype(BF16)
        sums = dot(jnp.concatenate([high, low], 1), ones)
        for half in range(2):
            lanes = slice(128 * half, 128 * half + 128)
            mine = row_f == rank_ref[c : c + 1, lanes]
            rows_out[0, c, :, lanes] = jnp.sum(jnp.where(mine, sums, 0.0), 0, keepdims=True)
    copy = pltpu.make_async_copy(rows_out, out, out_sem)
    copy.start()
    copy.wait()


VMEM_SPEC = pl.BlockSpec(memory_space=pltpu.VMEM)
HBM_SPEC = pl.BlockSpec(memory_space=pl.ANY)


def prepare(data, interpret=False):
    return pl.pallas_call(
        prep_kernel,
        out_shape=(
            jax.ShapeDtypeStruct((ROWS, KD), BF16),
            jax.ShapeDtypeStruct((NX, PS), F32),
            jax.ShapeDtypeStruct((24, 128), jnp.int32),
        ),
        in_specs=[VMEM_SPEC],
        out_specs=[VMEM_SPEC] * 3,
        scratch_shapes=[
            pltpu.VMEM((16 * STRIDE, 128), F32),
            pltpu.VMEM((16 * STRIDE, 128), F32),
            pltpu.VMEM((16, PS + MOVE, KD), F32),
            pltpu.VMEM((ROWS, KD), F32),
            pltpu.VMEM((24, 128), jnp.int32),
            pltpu.SMEM((24, 128), jnp.int32),
            pltpu.SemaphoreType.DMA,
        ],
        compiler_params=pltpu.CompilerParams(vmem_limit_bytes=40 << 20),
        interpret=interpret,
        name="prepare",
    )(data)


def pair_sums(pencils, fields, group, role, table, shift, inputs, targets, rest, interpret=False):
    n = len(pencils)
    out_shape = [jax.ShapeDtypeStruct((ROWS, 128), F32)] * 2
    out_specs = [VMEM_SPEC] * 2
    first_in, first_out = len(inputs) + 3, 0
    scratch = [
        pltpu.VMEM((n, 8, 48, 128), F32),
        pltpu.VMEM((n, RC * STRIDE, 128), F32),
        pltpu.VMEM((n, RC * STRIDE, 128), F32),
        pltpu.VMEM((n * RC, KD, PS), BF16),
        pltpu.VMEM((n * RC + 8, 128), F32),
        pltpu.VMEM((n * RC + 8, 128), F32),
        pltpu.VMEM((group, BLOCK, PS * len(fields)), F32),
    ]
    if role == "last":
        out_shape = [jax.ShapeDtypeStruct((1, NX, 1, PS), F32)] + out_shape
        first_in, first_out = first_in + 1, 1
        out_specs = [HBM_SPEC] + out_specs
        scratch = [pltpu.VMEM((NX, PS + MOVE, 128), F32), pltpu.VMEM((1, NX, 1, PS), F32), pltpu.SemaphoreType.DMA] + scratch
    scratch = scratch + [
        pltpu.SMEM((24 * 128,), jnp.int32),
        pltpu.SMEM((2,), jnp.int32),
        pltpu.SemaphoreType.DMA,
        pltpu.SemaphoreType.DMA,
    ]
    aliases = {} if role == "first" else {first_in: first_out, first_in + 1: first_out + 1}
    return pl.pallas_call(
        functools.partial(pair_kernel, pencils, fields, group, len(inputs), role),
        out_shape=out_shape,
        in_specs=[VMEM_SPEC] * (len(inputs) + 3 + len(rest)),
        out_specs=out_specs,
        scratch_shapes=scratch,
        input_output_aliases=aliases,
        compiler_params=pltpu.CompilerParams(vmem_limit_bytes=40 << 20),
        interpret=interpret,
    )(table, shift, *inputs, targets, *rest)


OWN = ((0, 0, 0, 0),)
SIDE = ((0, 0, -1, 0), (1, 0, 1, 0))
FAR = ((0, 0, 0, -1), (1, 0, 0, 1), (0, 1, -1, -1), (1, 1, -1, 1), (0, 2, 1, -1), (1, 2, 1, 1))


def own_sums(table, shift, data, targets):
    return pair_sums(OWN, (1,), 16, "first", table, shift, [data[None]], targets, [])


def side_sums(table, shift, below, above, targets, sums):
    return pair_sums(SIDE, (2,), 16, "next", table, shift, [below[None], above[None]], targets, sums)


def far_sums(table, shift, low, high, targets, rank, sums):
    return pair_sums(FAR, (3, 4), 8, "last", table, shift, [low, high], targets, [rank, *sums])[0]


def ring(axis, distance):
    count = lax.axis_size(axis)
    return [(i, (i + distance) % count) for i in range(count)]


def shards(positions, masses, counts, shear_offset):
    slot_index = lax.broadcasted_iota(jnp.int32, masses.shape, 3)
    weight = jnp.where(slot_index < counts[..., None], masses, jnp.float32(0.0))
    data = jnp.concatenate([positions, weight[None]], 0).reshape(4, NX, PS)
    index = lax.axis_index("shear")
    offset = shear_offset[0]
    shift = jnp.stack([
        jnp.where(index == 0, NX - offset, 0),
        jnp.where(index == lax.axis_size("shear") - 1, offset, 0),
    ]).astype(jnp.int32)
    below = lax.ppermute(data, "shear", ring("shear", 1))
    above = lax.ppermute(data, "shear", ring("shear", -1))
    targets, rank, table = prepare(data)
    table = table.reshape(-1)
    sums = own_sums(table, shift, data, targets)
    rows = jnp.stack([data, below, above])
    rows, targets, rank, table, shift, sums = lax.optimization_barrier((rows, targets, rank, table, shift, sums))
    low = lax.ppermute(rows, "cross", ring("cross", 1))
    high = lax.ppermute(rows, "cross", ring("cross", -1))
    sums = side_sums(table, shift, rows[1], rows[2], targets, sums)
    density = far_sums(table, shift, low, high, targets, rank, sums)
    return density


def solution(mesh):
    in_specs = (
        P(None, "shear", None, "cross", None),
        P("shear", None, "cross", None),
        P("shear", None, "cross"),
        P(),
    )
    out_specs = P("shear", None, "cross", None)
    return jax.shard_map(shards, mesh=mesh, in_specs=in_specs, out_specs=out_specs, check_vma=False)
```
